32 devices in a mesh: gx: 2 (over core), gy: 4 (over y, x), gz: 4 (over z).
Axes of the slice: x: 2, y: 2, z: 4, core: 2. Of those that a mesh axis runs over, the one named last changes fastest.
Arguments:
- velocity: float32 [3, 16, 64, 512], P(None, 'gx', 'gy', 'gz'), may hold values from -6 to 6
- diffusion: float32 [3], replicated, may hold values from 0.5 to 4
Outputs:
- viscous_velocity: float32 [3, 16, 64, 512], P(None, 'gx', 'gy', 'gz')
- residual: float32 [3, 16, 64, 512], P(None, 'gx', 'gy', 'gz')
The draws below stay inside these ranges and needn't reach their ends.
All inputs are finite; a program needn't handle non-finite values.
Results may differ from the reference program's by a relative error of at most 0.0003.
Values sent between devices are 32-bit elements; how exact they have to be, the bound alone decides.
A program may use at most 64 MiB of HBM per device.

```python
import math
import jax
import jax.numpy as jnp

ITERS = 3
NX = 16
NY = 64
NZ = 512


def level_of(stream_key, shape, cuts, least, top_value):
    def one(axis_at, parts):
        draws = jax.random.uniform(jax.random.fold_in(jax.random.fold_in(stream_key, 6), axis_at), (parts,), jnp.float32, least / len(cuts), top_value / len(cuts))
        return jnp.repeat(jnp.exp(draws), shape[axis_at] // parts).reshape((-1,) + (1,) * (len(shape) - axis_at - 1))

    loudness = one(*cuts[0])
    for cut in cuts[1:]:
        loudness = loudness * one(*cut)
    return loudness


def bell_draw(own_key, extent, width, limit, pieces=(), kind=jnp.bfloat16):
    result = width * jax.random.normal(own_key, extent, jnp.float32)
    if pieces:
        result = result * level_of(own_key, extent, pieces, -0.22, 0.18)
    return jnp.clip(result, -limit, limit).astype(kind)


def setup_inputs(seed: int = 0) -> dict:
    key_list = jax.random.split(jax.random.key(seed), 3)
    return {
        "velocity": bell_draw(key_list[0], (3, NX, NY, NZ), 1.0, 6.0, ((1, 2), (2, 4), (3, 4)), jnp.float32),
        "diffusion": jnp.clip(jnp.exp(jax.random.uniform(key_list[1], (3,), jnp.float32, math.log(0.5), math.log(4.0))), 0.5, 4.0),
    }


time_step = 0.25


def trimmed(array, axis, offset):
    index = [slice(None)] + [slice(1, -1)] * 3
    index[axis + 1] = slice(1 + offset, array.shape[axis + 1] - 1 + offset)
    return array[tuple(index)]


def advection(padded):
    total = None
    for axis in range(3):
        flux = padded[axis:axis + 1] * padded
        term = (trimmed(flux, axis, 1) - trimmed(flux, axis, -1)) * 0.5
        total = term if total is None else total + term
    return total


def operate(field, coefficient):
    padded = jnp.pad(field, ((0, 0), (1, 1), (1, 1), (1, 1)))
    beside = padded[:, 2:, 1:-1, 1:-1] + padded[:, :-2, 1:-1, 1:-1]
    beside = beside + padded[:, 1:-1, 2:, 1:-1] + padded[:, 1:-1, :-2, 1:-1]
    beside = beside + padded[:, 1:-1, 1:-1, 2:] + padded[:, 1:-1, 1:-1, :-2]
    return (1.0 + 6.0 * coefficient) * field - coefficient * beside


def inner(first, second):
    return jnp.sum(first * second, axis=(1, 2, 3))[:, None, None, None]


def reference(velocity, diffusion):
    coefficient = diffusion[:, None, None, None]
    padded = jnp.pad(velocity, ((0, 0), (1, 1), (1, 1), (1, 1)))
    section = velocity - time_step * advection(padded)
    solution = jnp.zeros_like(section)
    residual = section
    direction = section
    norm_now = inner(residual, residual)
    for iteration in range(ITERS):
        image = operate(direction, coefficient)
        step_size = norm_now / inner(direction, image)
        solution = solution + step_size * direction
        residual = residual - step_size * image
        norm_next = inner(residual, residual)
        direction = residual + (norm_next / norm_now) * direction
        norm_now = norm_next
    return solution, residual
```

```python
import functools
import itertools

import jax
import jax.numpy as jnp
from jax import lax
from jax.experimental import pallas as pl
from jax.experimental.pallas import tpu as pltpu
from jax.sharding import PartitionSpec as P

AXES = ("gx", "gy", "gz")
MESH_IDS = pl.DeviceIdType.MESH
MARGIN = 4
PAIRS = ((0, 0), (0, 1), (1, 1), (0, 2), (1, 2), (2, 2), (2, 3))
time_step = 0.25
ONE_SHOT = 64
GRANT = 66200000
SMALL = 4194304
EARLY = False


def around(sizes, moved):
    return tuple(lax.rem(lax.axis_index(a) + o, s) for a, o, s in zip(AXES, moved, sizes))


def groups_of(sizes):
    total = sizes[0] * sizes[1] * sizes[2]
    if total <= ONE_SHOT:
        return [(0, 1, 2)]
    return [(0,), (1,), (2,)]


def offsets_of(sizes, group):
    ranges = [range(sizes[k]) if k in group else range(1) for k in range(3)]
    return [o for o in itertools.product(*ranges) if any(o)]


def slot_of(sizes, group):
    slot = 0
    for k in group:
        slot = slot * sizes[k] + lax.axis_index(AXES[k])
    return slot


def kernel(sizes, diff_hbm, v_hbm, B0, B1, B2, B3, co_ref, diff_ref, V, S0, S1, S2, own, left_pack, right_pack, PX, low, high, mask_low, mask_high, row, *rest):
    groups = groups_of(sizes)
    gathered, (fs, fr, gs, gr, ins, waves) = rest[: len(groups)], rest[len(groups):]
    comps, X, Y, Z = v_hbm.shape
    M, D = MARGIN, MARGIN - 1
    XR, YR = X + 2 * M, Y + 2 * M
    tiles = Y // 8
    here = [lax.axis_index(a) for a in AXES]

    def exists(moved):
        ok = None
        for k in range(3):
            if moved[k]:
                place = here[k] + moved[k]
                one = (place >= 0) & (place < sizes[k])
                ok = one if ok is None else ok & one
        return ok

    def missing(moved):
        return pl.when(jnp.logical_not(exists(moved)))

    def shifted(moved):
        return tuple(h + m for h, m in zip(here, moved))

    peers = set()
    for group in groups:
        peers.update(offsets_of(sizes, group))
    for dx, dy in itertools.product((-1, 0, 1), (-1, 0, 1)):
        moved = (dx % sizes[0], dy % sizes[1], 0)
        if any(moved):
            peers.add(moved)
    peers = sorted(peers, key=lambda o: -sum(min(m, s - m) for m, s in zip(o, sizes)))
    barrier = pltpu.get_barrier_semaphore()
    relayed = len(groups) == 1
    greeted = [o for o in peers if not (relayed and o[2])]
    along_z = ((0, 0, -1), (0, 0, 1))
    last_wave = sizes[2] - 1 if relayed else 1

    own_cells = pltpu.make_async_copy(v_hbm, V.at[:, 0:X, 0:Y], ins.at[0])
    own_cells.start()
    own_diff = pltpu.make_async_copy(diff_hbm, diff_ref, ins.at[1])
    own_diff.start()

    expected = len(greeted)
    for moved in greeted:
        pl.semaphore_signal(barrier, inc=1, device_id=around(sizes, moved), device_id_type=MESH_IDS)
    for moved in along_z if relayed else ():
        @pl.when(exists(moved))
        def _(moved=moved):
            pl.semaphore_signal(barrier, inc=1, device_id=shifted(moved), device_id_type=MESH_IDS)

        expected = expected + exists(moved).astype(jnp.int32)

    def announce(wave):
        for k, moved in enumerate(along_z):
            @pl.when(exists(moved))
            def _(k=k, moved=moved):
                pl.semaphore_signal(waves.at[wave, k], inc=1, device_id=shifted(moved), device_id_type=MESH_IDS)

    def heard(wave):
        for k, moved in enumerate(along_z):
            @pl.when(exists(tuple(-m for m in moved)))
            def _(k=k):
                pl.semaphore_wait(waves.at[wave, k], 1)

    @missing((1, 0, 0))
    def _():
        V[:, X : X + M] = jnp.zeros((comps, M, YR, Z), jnp.float32)
        right_pack[...] = jnp.zeros((comps, Y, Z), jnp.float32)

    @missing((-1, 0, 0))
    def _():
        V[:, X + M : XR] = jnp.zeros((comps, M, YR, Z), jnp.float32)
        left_pack[...] = jnp.zeros((comps, Y, Z), jnp.float32)

    for dy, first_row in ((1, Y), (-1, Y + M)):
        @missing((0, dy, 0))
        def _(first_row=first_row):
            V[:, 0:X, first_row : first_row + M] = jnp.zeros((comps, X, M, Z), jnp.float32)
            PX[:, first_row : first_row + M] = jnp.zeros((comps, M, Z), jnp.float32)

    for dz, ref in ((-1, low), (1, high)):
        @missing((0, 0, dz))
        def _(ref=ref):
            ref[:, 0:Y] = jnp.zeros((comps, Y, Z), jnp.float32)

        for dy, first_row in ((1, Y), (-1, Y + M)):
            @missing((0, dy, dz))
            def _(ref=ref, first_row=first_row):
                ref[:, first_row : first_row + M] = jnp.zeros((comps, M, Z), jnp.float32)

    lane = lax.broadcasted_iota(jnp.int32, (8, Z), 1)
    lanes = lax.broadcasted_iota(jnp.int32, (YR, Z), 1)
    rows = lax.broadcasted_iota(jnp.int32, (YR, Z), 0)
    yy = jnp.where(rows >= Y + M, rows - YR, rows) + here[1] * Y
    xx = lanes // 8
    xx = jnp.where(xx >= X + M, xx - XR, xx) + here[0] * X
    inside = (yy >= 0) & (yy < Y * sizes[1]) & (xx >= 0) & (xx < X * sizes[0])
    depth = lanes % 8 - M
    mask_low[...] = jnp.where(inside & (depth + here[2] * Z >= 0), 1.0, 0.0).astype(jnp.float32)
    mask_high[...] = jnp.where(inside & (depth + here[2] * Z + Z < Z * sizes[2]), 1.0, 0.0).astype(jnp.float32)
    beyond = lax.broadcasted_iota(jnp.int32, (8, Z), 0)
    beyond = jnp.where(beyond < M, beyond + Y, beyond - 2 * M) + here[1] * Y
    y_mask = jnp.where((beyond >= 0) & (beyond < Y * sizes[1]), 1.0, 0.0).astype(jnp.float32)

    own_cells.wait()
    for c in range(comps):
        for t in range(tiles):
            packed = jnp.zeros((8, Z), jnp.float32)
            for x in range(X):
                rolled = pltpu.roll(V[c, x, 8 * t : 8 * t + 8], (8 * x + M) % Z, 1)
                packed = jnp.where(lane // 8 == x, rolled, packed)
            own[c, 8 * t : 8 * t + 8] = packed
    pl.semaphore_wait(barrier, expected)

    copies = []

    def plan(src, dst, moved):
        k = len(copies)
        copy = pltpu.make_async_remote_copy(
            src_ref=src, dst_ref=dst, send_sem=fs.at[k], recv_sem=fr.at[k],
            device_id=shifted(moved), device_id_type=MESH_IDS,
        )
        copies.append((copy, moved))
        return copy, moved

    def start(which, also=None):
        copy, moved = which
        ok = exists(moved)
        pl.when(ok if also is None else ok & also)(copy.start)

    def received(which):
        for copy, moved in which:
            pl.when(exists(tuple(-m for m in moved)))(copy.wait_recv)

    announce(1)
    x_packs = [plan(own, right_pack, (-1, 0, 0)), plan(own, left_pack, (1, 0, 0))]
    for which in x_packs:
        start(which)

    more = exists((1, 0, 0))
    begins = [jnp.where(more, X - M, 0), jnp.where(more, 0, X - M)]
    odd = lax.rem(here[1], 2) == 1
    y_faces = []
    for begin in begins:
        planes = pl.ds(begin, M)
        y_faces.append((
            plan(V.at[:, planes, 0:M], V.at[:, planes, Y : Y + M], (0, -1, 0)),
            plan(V.at[:, planes, Y - M : Y], V.at[:, planes, Y + M : YR], (0, 1, 0)),
        ))

    def start_faces(pair):
        start(pair[1], odd)
        start(pair[0])
        start(pair[1], jnp.logical_not(odd))

    start_faces(y_faces[0])
    x_faces = [
        plan(V.at[:, 0:M, 0:Y], V.at[:, X : X + M, 0:Y], (-1, 0, 0)),
        plan(V.at[:, X - M : X, 0:Y], V.at[:, X + M : XR, 0:Y], (1, 0, 0)),
    ]
    for which in x_faces:
        start(which)
    if EARLY:
        start_faces(y_faces[1])

    received(x_packs)
    for c in range(comps):
        for t in range(tiles):
            at = slice(8 * t, 8 * t + 8)
            beside_x = jnp.where(lane < 8 * M, right_pack[c, at], left_pack[c, at])
            PX[c, at] = jnp.where(lane < 8 * X, own[c, at], pltpu.roll(beside_x, 8 * X, 1))
    heard(1)
    z_copies = []
    for dz in (-1, 1, 0):
        ref = {1: low, -1: high, 0: PX}[dz]
        z_copies.append(plan(PX.at[:, 0:M], ref.at[:, Y : Y + M], (0, -1, dz)))
        z_copies.append(plan(PX.at[:, Y - M : Y], ref.at[:, Y + M : YR], (0, 1, dz)))
    z_copies.append(plan(PX.at[:, 0:Y], high.at[:, 0:Y], (0, 0, -1)))
    z_copies.append(plan(PX.at[:, 0:Y], low.at[:, 0:Y], (0, 0, 1)))
    for which in z_copies:
        start(which)
    if not EARLY:
        start_faces(y_faces[1])
    for wave in range(2, last_wave + 1):
        announce(wave)
        if wave < last_wave:
            heard(wave)

    forwards = [
        plan(V.at[:, 0:M, Y:YR], V.at[:, X : X + M, Y:YR], (-1, 0, 0)),
        plan(V.at[:, X - M : X, Y:YR], V.at[:, X + M : XR, Y:YR], (1, 0, 0)),
    ]
    received(y_faces[0])
    start(forwards[1])
    start(forwards[0], jnp.logical_not(more))
    received(y_faces[1])
    start(forwards[0], more)
    received(x_faces)
    received(z_copies)
    received(forwards)

    def up(f, by, axis):
        return pltpu.roll(f, f.shape[axis] - by, axis)

    def down(f, by, axis):
        return pltpu.roll(f, by, axis)

    quarter = 0.5 * time_step
    k_low = lanes % 8 < M
    strips = []
    seams = [[None] * comps for _ in range(4)]
    for side, mask in ((0, mask_low), (1, mask_high)):
        inner = mask[...]
        v = []
        for c in range(comps):
            if side == 0:
                v.append(jnp.where(k_low, low[c], PX[c]))
            else:
                v.append(jnp.where(k_low, PX[c], high[c]))
        fields = [[], [], [], []]
        for c in range(comps):
            fx, fy, fz = v[0] * v[c], v[1] * v[c], v[2] * v[c]
            total = up(fx, 8, 1) - down(fx, 8, 1)
            total = total + (up(fy, 1, 0) - down(fy, 1, 0))
            total = total + (up(fz, 1, 1) - down(fz, 1, 1))
            fields[0].append(fz)
            fields[1].append((v[c] - quarter * total) * inner)
        for c in range(comps):
            def around_strip(f):
                return (up(f, 8, 1) + down(f, 8, 1)) + (up(f, 1, 0) + down(f, 1, 0)) + (up(f, 1, 1) + down(f, 1, 1))

            fields[2].append(around_strip(fields[1][c]) * inner)
            fields[3].append(around_strip(fields[2][c]) * inner - 6.0 * fields[1][c])
        strips.append(fields)
    for k in range(4):
        for c in range(comps):
            seams[k][c] = jnp.where(k_low, up(strips[1][k][c], 1, 1), down(strips[0][k][c], 1, 1))

    def ring(i):
        return i % XR

    def z_pair(f, seam, i):
        edge = pltpu.roll(seam, (Z - 8 * ring(i) - M) % Z, 1)
        n = f.shape[0]
        at = lanes[0:n]
        after = jnp.where(at == Z - 1, edge[0:n], up(f, 1, 1))
        before = jnp.where(at == 0, edge[0:n], down(f, 1, 1))
        return after, before

    def masked(ref, c, i, value):
        at = ring(i)
        top, bottom = value[0:Y], value[Y:YR]
        if 0 <= i < X:
            ref[c, at, 0:Y] = top
            ref[c, at, Y:YR] = bottom * y_mask
        else:
            place = here[0] * X + i
            xin = jnp.where((place >= 0) & (place < X * sizes[0]), 1.0, 0.0).astype(jnp.float32)
            ref[c, at, 0:Y] = top * xin
            ref[c, at, Y:YR] = bottom * (y_mask * xin)

    for i in range(-D, X + D):
        at, after, before = ring(i), ring(i + 1), ring(i - 1)
        v = [V[c, at] for c in range(comps)]
        va = [V[c, after] for c in range(comps)]
        vb = [V[c, before] for c in range(comps)]
        for c in range(comps):
            total = va[0] * va[c] - vb[0] * vb[c]
            fy = v[1] * v[c]
            total = total + (up(fy, 1, 0) - down(fy, 1, 0))
            fa, fb = z_pair(v[2] * v[c], seams[0][c], i)
            total = total + (fa - fb)
            masked(S0, c, i, v[c] - quarter * total)

    def beside(ref, seam, c, i):
        f = ref[c, ring(i)]
        total = ref[c, ring(i + 1)] + ref[c, ring(i - 1)]
        total = total + (up(f, 1, 0) + down(f, 1, 0))
        fa, fb = z_pair(f, seam, i)
        return total + (fa + fb)

    def folded(value):
        part = value[0:8]
        for t in range(1, tiles):
            part = part + value[8 * t : 8 * t + 8]
        return part

    def masked_less(ref, c, i, value, less):
        at = ring(i)
        if 0 <= i < X:
            ref[c, at, 0:Y] = value[0:Y] - less[0:Y]
            ref[c, at, Y:YR] = value[Y:YR] * y_mask - less[Y:YR]
        else:
            place = here[0] * X + i
            xin = jnp.where((place >= 0) & (place < X * sizes[0]), 1.0, 0.0).astype(jnp.float32)
            ref[c, at, 0:Y] = value[0:Y] * xin - less[0:Y]
            ref[c, at, Y:YR] = value[Y:YR] * (y_mask * xin) - less[Y:YR]

    sums = [None] * (len(PAIRS) * comps)

    def first(c, i):
        masked(S1, c, i, beside(S0, seams[1][c], c, i))

    def second(c, i):
        masked_less(S2, c, i, beside(S1, seams[2][c], c, i), 6.0 * S0[c, ring(i)])

    def third(c, i):
        p = [S[c, i, 0:Y] for S in (S0, S1, S2)]
        f = S2[c, i]
        edge = pltpu.roll(seams[3][c], (Z - 8 * i - M) % Z, 1)
        fa = jnp.where(lanes[0:Y] == Z - 1, edge[0:Y], up(f[0:Y], 1, 1))
        p.append(S2[c, ring(i + 1), 0:Y] + up(f, 1, 0)[0:Y] + fa)
        for k, (a, b) in enumerate(PAIRS):
            part = folded(p[a] * p[b])
            at = k * comps + c
            sums[at] = part if sums[at] is None else sums[at] + part

    for i in range(-2, X + 2):
        for c in range(comps):
            first(c, i)
    for i in range(-1, X + 1):
        for c in range(comps):
            second(c, i)
    for i in range(X):
        for c in range(comps):
            third(c, i)
    line = jnp.zeros((8, Z), jnp.float32)
    for k, part in enumerate(sums):
        line = jnp.where(lane == k, jnp.sum(part, axis=1, keepdims=True), line)
    line = jnp.sum(line, axis=0, keepdims=True)

    if last_wave >= 2:
        heard(last_wave)

    def residual_basis():
        for c in range(comps):
            for i in range(X):
                B3[c, i] = beside(S2, seams[3][c], c, i)[0:Y] - 9.0 * S1[c, i, 0:Y]
                for B, S in ((B0, S0), (B1, S1), (B2, S2)):
                    B[c, i] = S[c, i, 0:Y]

    order = 0
    for group, landing in zip(groups, gathered):
        mine = slot_of(sizes, group)
        row[...] = line
        landing[mine] = line
        offsets = [o for o in peers if o in offsets_of(sizes, group)]
        for moved in offsets:
            pltpu.make_async_remote_copy(
                src_ref=row, dst_ref=landing.at[mine], send_sem=gs.at[order], recv_sem=gr.at[order],
                device_id=around(sizes, moved), device_id_type=MESH_IDS,
            ).start()
        if order == 0:
            residual_basis()
        many = landing.at[pl.ds(0, len(offsets))]
        pltpu.make_async_copy(many, many, gr.at[order]).wait()
        line = landing[0]
        for k in range(1, len(offsets) + 1):
            line = line + landing[k]
        pltpu.make_async_copy(many, many, gs.at[order]).wait()
        order += 1

    g = {}
    for k, (a, b) in enumerate(PAIRS):
        value = line if k == 0 else pltpu.roll(line, Z - k * comps, 1)
        g[a, b] = g[b, a] = value
    g[2, 3] = g[3, 2] = 2.0 * g[2, 3] - 9.0 * g[1, 2]
    g[0, 3] = g[1, 2] - 9.0 * g[0, 1]
    g[1, 3] = g[2, 2] + 6.0 * g[0, 2] - 9.0 * g[1, 1]
    at_lane = lax.broadcasted_iota(jnp.int32, (1, Z), 1)
    own_diff.wait()
    coef = jnp.full((1, Z), 1.0, jnp.float32)
    for c in range(comps):
        coef = jnp.where(at_lane == c, diff_ref[c], coef)
    diagonal = 1.0 + 6.0 * coef
    zero = jnp.zeros((1, Z), jnp.float32)

    def image_of(d):
        return [
            diagonal * d[0] - 6.0 * coef * d[1],
            diagonal * d[1] - coef * (d[0] + 9.0 * d[2]),
            diagonal * d[2] - coef * d[1],
            -coef * d[2],
        ]

    def form(a, b):
        total = None
        for i, left in enumerate(a):
            for j, right in enumerate(b):
                if left is zero or right is zero:
                    continue
                term = left * right * g[i, j]
                total = term if total is None else total + term
        return total

    res = [zero + 1.0, zero, zero, zero]
    direction = [zero + 1.0, zero, zero]
    found = [zero, zero, zero]
    norm = g[0, 0]
    for iteration in range(3):
        image = image_of(direction)
        if iteration == 0:
            image = [image[0], image[1], zero, zero]
        elif iteration == 1:
            image = [image[0], image[1], image[2], zero]
        step = norm / form(direction, image)
        found = [f if d is zero else f + step * d for f, d in zip(found, direction)]
        res = [r if m is zero else r - step * m for r, m in zip(res, image)]
        if iteration < 2:
            after = form(res[:3], res[:3])
            ratio = after / norm
            direction = [r if d is zero else r + ratio * d for r, d in zip(res, direction)]
            norm = after

    for k, value in enumerate(found + res):
        co_ref[k : k + 1] = value

    for copy, moved in copies:
        pl.when(exists(moved))(copy.wait_send)


def combine(co_ref, B0, B1, B2, B3, x_hbm, r_hbm, x_ref, r_ref, sems):
    comps, X, Y, Z = B0.shape
    at_lane = lax.broadcasted_iota(jnp.int32, (8, Z), 1)
    table = co_ref[...]
    copies = []
    for c in range(comps):
        column = jnp.sum(jnp.where(at_lane == c, table, 0.0), axis=1, keepdims=True)
        f = [jnp.broadcast_to(column[k : k + 1], (Y, Z)) for k in range(7)]
        for x in range(X):
            p = [B[c, x] for B in (B0, B1, B2, B3)]
            x_ref[c, x] = f[0] * p[0] + f[1] * p[1] + f[2] * p[2]
            r_ref[c, x] = f[3] * p[0] + f[4] * p[1] + f[5] * p[2] + f[6] * p[3]
        for k, (src, dst) in enumerate(((x_ref, x_hbm), (r_ref, r_hbm))):
            copy = pltpu.make_async_copy(src.at[c], dst.at[c], sems.at[k, c])
            copy.start()
            copies.append(copy)
    for copy in copies:
        copy.wait()


def solution(mesh):
    sizes = tuple(mesh.shape[a] for a in AXES)
    groups = groups_of(sizes)

    def body(velocity, diffusion):
        comps, X, Y, Z = velocity.shape
        XR, YR = X + 2 * MARGIN, Y + 2 * MARGIN
        assert X == 2 * MARGIN and XR * 8 == Z and MARGIN * 2 == 8
        f32 = jnp.float32
        whole = pltpu.VMEM((comps, XR, YR, Z), f32)
        packed = pltpu.VMEM((comps, Y, Z), f32)
        strip = pltpu.VMEM((comps, YR, Z), f32)
        counts = [len(offsets_of(sizes, group)) + 1 for group in groups]
        out = pltpu.VMEM(velocity.shape, f32)
        vmem = pl.BlockSpec(memory_space=pltpu.VMEM)
        hbm = pl.BlockSpec(memory_space=pltpu.HBM)
        basis = pl.pallas_call(
            functools.partial(kernel, sizes),
            out_shape=(out, out, out, out, pltpu.VMEM((8, Z), f32)),
            in_specs=[hbm] * 2,
            out_specs=(vmem,) * 5,
            scratch_shapes=[
                pltpu.SMEM((comps,), f32),
                whole, whole, whole, whole,
                packed, packed, packed,
                strip, strip, strip,
                pltpu.VMEM((YR, Z), f32),
                pltpu.VMEM((YR, Z), f32),
                pltpu.VMEM((1, Z), f32),
                *[pltpu.VMEM((count, 1, Z), f32) for count in counts],
                pltpu.SemaphoreType.DMA((18,)),
                pltpu.SemaphoreType.DMA((18,)),
                pltpu.SemaphoreType.DMA((len(groups),)),
                pltpu.SemaphoreType.DMA((len(groups),)),
                pltpu.SemaphoreType.DMA((2,)),
                pltpu.SemaphoreType.REGULAR((sizes[2] + 1, 2)),
            ],
            compiler_params=pltpu.CompilerParams(collective_id=0, has_side_effects=True, vmem_limit_bytes=GRANT),
        )(diffusion, velocity)
        shape = jax.ShapeDtypeStruct(velocity.shape, f32)
        return pl.pallas_call(
            combine,
            out_shape=(shape, shape),
            in_specs=[vmem] * 5,
            out_specs=(hbm, hbm),
            scratch_shapes=[
                pltpu.VMEM(velocity.shape, f32),
                pltpu.VMEM(velocity.shape, f32),
                pltpu.SemaphoreType.DMA((2, comps)),
            ],
            compiler_params=pltpu.CompilerParams(vmem_limit_bytes=SMALL),
        )(basis[4], *basis[:4])

    return jax.shard_map(
        body,
        mesh=mesh,
        in_specs=(P(None, "gx", "gy", "gz"), P()),
        out_specs=(P(None, "gx", "gy", "gz"), P(None, "gx", "gy", "gz")),
        check_vma=False,
    )
```

```python
import functools
import itertools

import jax
import jax.numpy as jnp
from jax import lax
from jax.experimental import pallas as pl
from jax.experimental.pallas import tpu as pltpu
from jax.sharding import PartitionSpec as P

AXES = ("gx", "gy", "gz")
MESH_IDS = pl.DeviceIdType.MESH
MARGIN = 4
PAIRS = ((0, 0), (0, 1), (1, 1), (0, 2), (1, 2), (2, 2), (2, 3))
time_step = 0.25
ONE_SHOT = 64
GRANT = 66200000
SMALL = 4194304
EARLY = False


def around(sizes, moved):
    return tuple(lax.rem(lax.axis_index(a) + o, s) for a, o, s in zip(AXES, moved, sizes))


def groups_of(sizes):
    total = sizes[0] * sizes[1] * sizes[2]
    if total <= ONE_SHOT:
        return [(0, 1, 2)]
    return [(0,), (1,), (2,)]


def offsets_of(sizes, group):
    ranges = [range(sizes[k]) if k in group else range(1) for k in range(3)]
    return [o for o in itertools.product(*ranges) if any(o)]


def slot_of(sizes, group):
    slot = 0
    for k in group:
        slot = slot * sizes[k] + lax.axis_index(AXES[k])
    return slot


def kernel(sizes, diff_hbm, v_hbm, B0, B1, B2, B3, co_ref, diff_ref, V, S0, S1, S2, D0, C0, D1, C1, D2, own, left_pack, right_pack, PX, WU, WD, low, high, mask_low, mask_high, row, *rest):
    groups = groups_of(sizes)
    gathered, (fs, fr, gs, gr, ins, waves) = rest[: len(groups)], rest[len(groups):]
    comps, X, Y, Z = v_hbm.shape
    M, D = MARGIN, MARGIN - 1
    XR, YR = X + 2 * M, Y + 2 * M
    tiles = Y // 8
    here = [lax.axis_index(a) for a in AXES]

    def exists(moved):
        ok = None
        for k in range(3):
            if moved[k]:
                place = here[k] + moved[k]
                one = (place >= 0) & (place < sizes[k])
                ok = one if ok is None else ok & one
        return ok

    def missing(moved):
        return pl.when(jnp.logical_not(exists(moved)))

    def shifted(moved):
        return tuple(h + m for h, m in zip(here, moved))

    peers = set()
    for group in groups:
        peers.update(offsets_of(sizes, group))
    for dx, dy in itertools.product((-1, 0, 1), (-1, 0, 1)):
        moved = (dx % sizes[0], dy % sizes[1], 0)
        if any(moved):
            peers.add(moved)
    peers = sorted(peers, key=lambda o: -sum(min(m, s - m) for m, s in zip(o, sizes)))
    barrier = pltpu.get_barrier_semaphore()
    relayed = len(groups) == 1
    greeted = [o for o in peers if not (relayed and o[2])]
    along_z = ((0, 0, -1), (0, 0, 1))
    last_wave = sizes[2] - 1 if relayed else 1

    own_cells = pltpu.make_async_copy(v_hbm, V.at[:, 0:X, 0:Y], ins.at[0])
    own_cells.start()
    own_diff = pltpu.make_async_copy(diff_hbm, diff_ref, ins.at[1])
    own_diff.start()

    expected = len(greeted)
    for moved in greeted:
        pl.semaphore_signal(barrier, inc=1, device_id=around(sizes, moved), device_id_type=MESH_IDS)
    for moved in along_z if relayed else ():
        @pl.when(exists(moved))
        def _(moved=moved):
            pl.semaphore_signal(barrier, inc=1, device_id=shifted(moved), device_id_type=MESH_IDS)

        expected = expected + exists(moved).astype(jnp.int32)

    def announce(wave):
        for k, moved in enumerate(along_z):
            @pl.when(exists(moved))
            def _(k=k, moved=moved):
                pl.semaphore_signal(waves.at[wave, k], inc=1, device_id=shifted(moved), device_id_type=MESH_IDS)

    def heard(wave):
        for k, moved in enumerate(along_z):
            @pl.when(exists(tuple(-m for m in moved)))
            def _(k=k):
                pl.semaphore_wait(waves.at[wave, k], 1)

    @missing((1, 0, 0))
    def _():
        V[:, X : X + M] = jnp.zeros((comps, M, YR, Z), jnp.float32)
        right_pack[...] = jnp.zeros((comps, Y, Z), jnp.float32)

    @missing((-1, 0, 0))
    def _():
        V[:, X + M : XR] = jnp.zeros((comps, M, YR, Z), jnp.float32)
        left_pack[...] = jnp.zeros((comps, Y, Z), jnp.float32)

    for dy, first_row in ((1, Y), (-1, Y + M)):
        @missing((0, dy, 0))
        def _(first_row=first_row):
            V[:, 0:X, first_row : first_row + M] = jnp.zeros((comps, X, M, Z), jnp.float32)

    for dz, ref in ((-1, low), (1, high)):
        @missing((0, 0, dz))
        def _(ref=ref):
            ref[:, 0:Y] = jnp.zeros((2, Y, Z), jnp.float32)

        for dy, first_row in ((1, Y), (-1, Y + M)):
            @missing((0, dy, dz))
            def _(ref=ref, first_row=first_row):
                ref[:, first_row : first_row + M] = jnp.zeros((2, M, Z), jnp.float32)

    lane = lax.broadcasted_iota(jnp.int32, (8, Z), 1)
    lanes = lax.broadcasted_iota(jnp.int32, (YR, Z), 1)
    k_low = lanes % 8 < M
    sub = lax.broadcasted_iota(jnp.int32, (8, Z), 0)
    xx = lane // 8
    xx = jnp.where(xx >= X + M, xx - XR, xx) + here[0] * X
    inside = (xx >= 0) & (xx < X * sizes[0])
    depth = lane % 8 - M
    mask_low[...] = jnp.where(inside & (depth + here[2] * Z >= 0), 1.0, 0.0).astype(jnp.float32)
    mask_high[...] = jnp.where(inside & (depth + here[2] * Z + Z < Z * sizes[2]), 1.0, 0.0).astype(jnp.float32)
    above = jnp.where(exists((0, 1, 0)), 1.0, 0.0).astype(jnp.float32)
    below = jnp.where(exists((0, -1, 0)), 1.0, 0.0).astype(jnp.float32)
    frame_mask = jnp.where(sub < M, above, below)
    one_sided = sizes[0] == 2
    for dx, ring_at in ((1, X), (-1, XR - 1)):
        @missing((dx, 0, 0))
        def _(ring_at=ring_at):
            for ref in (S0, S1, S2, C0, C1, D2):
                ref[:, ring_at] = jnp.zeros((comps,) + ref.shape[2:], jnp.float32)

    own_cells.wait()
    for c in range(comps):
        for t in range(tiles):
            packed = jnp.zeros((8, Z), jnp.float32)
            for x in range(X):
                rolled = pltpu.roll(V[c, x, 8 * t : 8 * t + 8], (8 * x + M) % Z, 1)
                packed = jnp.where(lane // 8 == x, rolled, packed)
            own[c, 8 * t : 8 * t + 8] = packed
    pl.semaphore_wait(barrier, expected)

    copies = []

    def plan(src, dst, moved):
        k = len(copies)
        copy = pltpu.make_async_remote_copy(
            src_ref=src, dst_ref=dst, send_sem=fs.at[k], recv_sem=fr.at[k],
            device_id=shifted(moved), device_id_type=MESH_IDS,
        )
        copies.append((copy, moved))
        return copy, moved

    def start(which, also=None):
        copy, moved = which
        ok = exists(moved)
        pl.when(ok if also is None else ok & also)(copy.start)

    def received(which):
        for copy, moved in which:
            pl.when(exists(tuple(-m for m in moved)))(copy.wait_recv)

    announce(1)
    x_packs = [plan(own, right_pack, (-1, 0, 0)), plan(own, left_pack, (1, 0, 0))]
    for which in x_packs:
        start(which)

    more = exists((1, 0, 0))
    begins = [jnp.where(more, X - M, 0), jnp.where(more, 0, X - M)]
    odd = lax.rem(here[1], 2) == 1
    y_faces = []
    for begin in begins:
        planes = pl.ds(begin, M)
        y_faces.append((
            plan(V.at[:, planes, 0:M], V.at[:, planes, Y : Y + M], (0, -1, 0)),
            plan(V.at[:, planes, Y - M : Y], V.at[:, planes, Y + M : YR], (0, 1, 0)),
        ))

    def start_far(pair):
        start(pair[1], odd)
        start(pair[0], jnp.logical_not(odd))

    def start_near(pair):
        start(pair[0], odd)
        start(pair[1], jnp.logical_not(odd))

    start_far(y_faces[0])
    start_near(y_faces[0])
    start_far(y_faces[1])
    x_faces = [
        plan(V.at[:, 0:M, 0:Y], V.at[:, X : X + M, 0:Y], (-1, 0, 0)),
        plan(V.at[:, X - M : X, 0:Y], V.at[:, X + M : XR, 0:Y], (1, 0, 0)),
    ]
    for which in x_faces:
        start(which)

    received(x_packs)
    for t in range(tiles):
        at = slice(8 * t, 8 * t + 8)
        px = []
        for c in range(comps):
            beside_x = jnp.where(lane < 8 * M, right_pack[c, at], left_pack[c, at])
            px.append(jnp.where(lane < 8 * X, own[c, at], pltpu.roll(beside_x, 8 * X, 1)))
            PX[c, at] = px[c]
        WU[0, at] = jnp.where(k_low[0:8], px[0], pltpu.roll(px[1], M, 1))
        WD[0, at] = jnp.where(k_low[0:8], pltpu.roll(px[1], Z - M, 1), px[0])
        WU[1, at] = px[2]
        WD[1, at] = px[2]
    z_edges, z_faces = [], []
    for dz, W, ref in ((-1, WD, high), (1, WU, low)):
        z_faces.append(plan(W, ref.at[:, 0:Y], (0, 0, dz)))
        start(z_faces[-1])
    heard(1)
    for dz, W, ref in ((-1, WD, high), (1, WU, low)):
        z_edges.append(plan(W.at[:, 0:M], ref.at[:, Y : Y + M], (0, -1, dz)))
        z_edges.append(plan(W.at[:, Y - M : Y], ref.at[:, Y + M : YR], (0, 1, dz)))
    for which in z_edges:
        start(which)
    start_near(y_faces[1])
    if last_wave >= 2:
        announce(2)
    quarter = 0.5 * time_step
    low_lane = k_low[0:8]
    zero8 = jnp.zeros((8, Z), jnp.float32)

    def split(f):
        return [f[8 * t : 8 * t + 8] for t in range(tiles)]

    def joined(ts):
        return jnp.concatenate(ts, axis=0)

    def up(f, by):
        return pltpu.roll(f, Z - by, 1)

    def down(f, by):
        return pltpu.roll(f, by, 1)

    def slide(f, by):
        return pltpu.roll(f, by % 8, 0)

    def rows_after(ts, last=0.0):
        r = [slide(t, -1) for t in ts] + [last]
        return [jnp.where(sub == 7, r[t + 1], r[t]) for t in range(len(ts))]

    def rows_before(ts, first=0.0):
        r = [first] + [slide(t, 1) for t in ts]
        return [jnp.where(sub == 0, r[t], r[t + 1]) for t in range(len(ts))]

    def inward(f):
        f = jnp.where(sub < M, slide(f, 1), slide(f, -1))
        return jnp.where((sub == 0) | (sub == 7), 0.0, f)

    def edge_of(seam, at):
        return pltpu.roll(seam, (Z - M) - 8 * at, 1)

    def seam_of(low_field, high_field):
        return jnp.where(low_lane, up(high_field, 1), down(low_field, 1))

    def planes_of(reach):
        own_planes = [(i, (i + 1) % XR, (i - 1) % XR, None) for i in range(X)]
        outer = []
        for j in range(reach):
            if one_sided:
                outer.append((
                    jnp.where(more, X + j, XR - 1 - j),
                    jnp.where(more, X + j + 1, (XR - j) % XR),
                    jnp.where(more, X + j - 1, XR - 2 - j),
                    None,
                ))
            else:
                for i in (X + j, -1 - j):
                    place = here[0] * X + i
                    xin = jnp.where((place >= 0) & (place < X * sizes[0]), 1.0, 0.0).astype(jnp.float32)
                    outer.append((i % XR, (i + 1) % XR, (i - 1) % XR, xin))
        return own_planes + outer

    def cut(value, xin):
        return value if xin is None else value * xin

    received(x_faces)
    for at, after, before, xin in planes_of(D):
        v = [split(V[c, at, 0:Y]) for c in range(comps)]
        va = [split(V[c, after, 0:Y]) for c in range(comps)]
        vb = [split(V[c, before, 0:Y]) for c in range(comps)]
        for c in range(comps):
            fy = [v[1][t] * v[c][t] for t in range(tiles)]
            ya, yb = rows_after(fy), rows_before(fy)
            for t in range(tiles):
                fz = v[2][t] * v[c][t]
                total = va[0][t] * va[c][t] - vb[0][t] * vb[c][t]
                total = total + (ya[t] - yb[t])
                za = jnp.where(lane == Z - 1, 0.0, up(fz, 1))
                zb = jnp.where(lane == 0, 0.0, down(fz, 1))
                total = total + (za - zb)
                S0[c, at, 8 * t : 8 * t + 8] = cut(v[c][t] - quarter * total, xin)

    for wave in range(2, last_wave):
        heard(wave)
        announce(wave + 1)

    forwards = [
        plan(V.at[:, 0:M, Y:YR], V.at[:, X : X + M, Y:YR], (-1, 0, 0)),
        plan(V.at[:, X - M : X, Y:YR], V.at[:, X + M : XR, Y:YR], (1, 0, 0)),
    ]
    received(y_faces[0])
    start(forwards[1])
    start(forwards[0], jnp.logical_not(more))
    received(z_faces)

    masks = [mask_low[...], mask_high[...]]
    strip_v = [[], []]
    for t in range(tiles):
        at = slice(8 * t, 8 * t + 8)
        outer = (low[0, at], up(low[0, at], M), low[1, at])
        strip_v[0].append([jnp.where(low_lane, outer[c], PX[c, at]) for c in range(comps)])
        outer = (high[0, at], down(high[0, at], M), high[1, at])
        strip_v[1].append([jnp.where(low_lane, PX[c, at], outer[c]) for c in range(comps)])
    strips = [[[None] * comps for _ in range(4)] for _ in range(2)]
    for side in range(2):
        v = strip_v[side]
        inner = masks[side]
        for c in range(comps):
            fy = [v[t][1] * v[t][c] for t in range(tiles)]
            ya, yb = rows_after(fy), rows_before(fy)
            fields = [[], []]
            for t in range(tiles):
                fx, fz = v[t][0] * v[t][c], v[t][2] * v[t][c]
                total = up(fx, 8) - down(fx, 8)
                total = total + (ya[t] - yb[t])
                total = total + (up(fz, 1) - down(fz, 1))
                fields[0].append(fz)
                fields[1].append((v[t][c] - quarter * total) * inner)
            strips[side][0][c], strips[side][1][c] = fields
        for k in (2, 3):
            for c in range(comps):
                f = strips[side][k - 1][c]
                ya, yb = rows_after(f), rows_before(f)
                out = []
                for t in range(tiles):
                    total = (up(f[t], 8) + down(f[t], 8)) + (ya[t] + yb[t]) + (up(f[t], 1) + down(f[t], 1))
                    total = total * inner
                    out.append(total if k == 2 else total - 6.0 * strips[side][1][c][t])
                strips[side][k][c] = out

    def seams_of(k):
        return [[seam_of(strips[0][k][c][t], strips[1][k][c][t]) for t in range(tiles)] for c in range(comps)]

    flip = jnp.where(lane % 8 < M, quarter, -quarter)
    border = (lane == 0) | (lane == Z - 1)
    seam = [[s * flip for s in ts] for ts in seams_of(0)]
    for at, after, before, xin in planes_of(D):
        for c in range(comps):
            for t in range(tiles):
                edge = cut(edge_of(seam[c][t], at), xin)
                rows = slice(8 * t, 8 * t + 8)
                S0[c, at, rows] = S0[c, at, rows] - jnp.where(border, edge, 0.0)

    def around_tiles(ref, seam, c, at, after, before, first=0.0, last=0.0):
        f = split(ref[c, at])
        fa, fb = split(ref[c, after]), split(ref[c, before])
        ya, yb = rows_after(f, last), rows_before(f, first)
        out = []
        for t in range(tiles):
            edge = edge_of(seam[c][t], at)
            za = jnp.where(lane == Z - 1, edge, up(f[t], 1))
            zb = jnp.where(lane == 0, edge, down(f[t], 1))
            out.append((fa[t] + fb[t]) + (ya[t] + yb[t]) + (za + zb))
        return out

    seam = seams_of(1)
    for at, after, before, xin in planes_of(2):
        for c in range(comps):
            out = around_tiles(S0, seam, c, at, after, before)
            for t in range(tiles):
                S1[c, at, 8 * t : 8 * t + 8] = cut(out[t], xin)
    seam = seams_of(2)
    for at, after, before, xin in planes_of(1):
        for c in range(comps):
            out = around_tiles(S1, seam, c, at, after, before)
            for t in range(tiles):
                rows = slice(8 * t, 8 * t + 8)
                S2[c, at, rows] = cut(out[t], xin) - 6.0 * S0[c, at, rows]

    sums = [None] * (len(PAIRS) * comps)

    def add(c, full, kept):
        for k, (a, b) in enumerate(PAIRS):
            part = None
            for left, right in zip(kept[a], full[b]):
                part = left * right if part is None else part + left * right
            at = k * comps + c
            sums[at] = part if sums[at] is None else sums[at] + part

    seam = [[up(strips[1][3][c][t], 1) for t in range(tiles)] for c in range(comps)]
    middle = [sub >= 3 if t == 0 else None for t in range(tiles)]
    last_tile = tiles - 1
    for i in range(X):
        for c in range(comps):
            full = [split(S[c, i]) for S in (S0, S1, S2)]
            f = full[2]
            fa = split(S2[c, i + 1])
            ya = rows_after(f)
            ya[last_tile] = jnp.where(sub < 4, ya[last_tile], 0.0)
            out = []
            for t in range(tiles):
                za = jnp.where(lane == Z - 1, edge_of(seam[c][t], i), up(f[t], 1))
                out.append(fa[t] + ya[t] + za)
            kept = []
            for a in range(3):
                ts = list(full[a])
                ts[0] = jnp.where(sub >= 3, ts[0], 0.0)
                ts[last_tile] = jnp.where(sub < 5, ts[last_tile], 0.0)
                kept.append(ts)
            add(c, full + [out], kept)

    received(y_faces[1])
    start(forwards[0], more)
    received(forwards)
    packed2 = []
    for c in range(comps):
        packed = zero8
        for x in range(XR):
            rolled = pltpu.roll(V[c, x, Y:YR], (8 * x + M) % Z, 1)
            packed = jnp.where(lane // 8 == x, rolled, packed)
        packed2.append(packed)
    received(z_edges)

    ends = (sub == 0) | (sub == 7)
    signed = jnp.where(sub == 0, -quarter, quarter)

    def frame_of(center, corr):
        f = jnp.where(sub < M, slide(center, 1), slide(center, -1))
        return jnp.where(ends, corr, f)

    def frame_section(v0, v2, v1, c, fx_part, z_part, inner):
        fy2 = v2[1] * v2[c]
        ya = jnp.where(sub == 7, slide(v0[1] * v0[c], -1), slide(fy2, -1))
        yb = jnp.where(sub == 0, slide(v1[1] * v1[c], 1), slide(fy2, 1))
        value = (v2[c] - quarter * (fx_part + (ya - yb) + z_part)) * inner
        return frame_of(value, signed * fy2)

    def from_tiles(first, last, by_first, by_last, at_first, at_last):
        return jnp.where(sub == at_last, slide(last, by_last), jnp.where(sub == at_first, slide(first, by_first), 0.0))

    at = slice(Y, YR)
    outer = (low[0, at], up(low[0, at], M), low[1, at])
    strip_v[0].append([jnp.where(low_lane, outer[c], packed2[c]) for c in range(comps)])
    outer = (high[0, at], down(high[0, at], M), high[1, at])
    strip_v[1].append([jnp.where(low_lane, packed2[c], outer[c]) for c in range(comps)])
    frames = [dict() for _ in range(2)]
    for side in range(2):
        v = strip_v[side]
        inner = masks[side] * frame_mask
        for c in range(comps):
            v2 = v[tiles]
            fx, fz = v2[0] * v2[c], v2[2] * v2[c]
            frames[side]["fz", c] = fz
            f0 = frame_section(v[0], v2, v[last_tile], c, up(fx, 8) - down(fx, 8), up(fz, 1) - down(fz, 1), inner)
            f0 = jnp.where(ends, f0 * masks[side], f0)
            c0 = inward(f0)
            s = strips[side]
            f1 = (up(c0, 8) + down(c0, 8)) + (up(c0, 1) + down(c0, 1)) + f0 + inward(c0)
            f1 = (f1 + from_tiles(s[1][c][0], s[1][c][last_tile], 5, 3, 5, 2)) * inner
            c1 = inward(f1)
            f2 = (up(c1, 8) + down(c1, 8)) + (up(c1, 1) + down(c1, 1)) + f1 + inward(c1)
            f2 = (f2 + from_tiles(s[2][c][0], s[2][c][last_tile], 4, 4, 4, 3)) * inner - 6.0 * inward(c0)
            frames[side]["c0", c], frames[side]["c1", c], frames[side]["f2", c] = c0, c1, f2

    def frame_seam(name, c):
        return seam_of(frames[0][name, c], frames[1][name, c])

    seam = [frame_seam("fz", c) for c in range(comps)]
    for at, after, before, xin in planes_of(D):
        v2 = [V[c, at, Y:YR] for c in range(comps)]
        va = [V[c, after, Y:YR] for c in range(comps)]
        vb = [V[c, before, Y:YR] for c in range(comps)]
        v0 = [V[c, at, 0:8] for c in range(comps)]
        v1 = [V[c, at, Y - 8 : Y] for c in range(comps)]
        for c in range(comps):
            fz = v2[2] * v2[c]
            edge = edge_of(seam[c], at)
            z_part = jnp.where(lane == Z - 1, edge, up(fz, 1)) - jnp.where(lane == 0, edge, down(fz, 1))
            f0 = frame_section(v0, v2, v1, c, va[0] * va[c] - vb[0] * vb[c], z_part, frame_mask)
            f0 = cut(f0, xin)
            D0[c, at] = f0
            C0[c, at] = inward(f0)

    def around_frame(C, seam, c, at, after, before):
        f = C[c, at]
        edge = edge_of(seam[c], at)
        za = jnp.where(lane == Z - 1, edge, up(f, 1))
        zb = jnp.where(lane == 0, edge, down(f, 1))
        return (C[c, after] + C[c, before]) + (za + zb) + inward(f)

    seam = [frame_seam("c0", c) for c in range(comps)]
    for at, after, before, xin in planes_of(2):
        for c in range(comps):
            f1 = around_frame(C0, seam, c, at, after, before) + D0[c, at]
            f1 = f1 + from_tiles(S0[c, at, 0:8], S0[c, at, Y - 8 : Y], 5, 3, 5, 2)
            f1 = cut(f1 * frame_mask, xin)
            D1[c, at] = f1
            C1[c, at] = inward(f1)
    seam = [frame_seam("c1", c) for c in range(comps)]
    for at, after, before, xin in planes_of(1):
        for c in range(comps):
            f2 = around_frame(C1, seam, c, at, after, before) + D1[c, at]
            f2 = f2 + from_tiles(S1[c, at, 0:8], S1[c, at, Y - 8 : Y], 4, 4, 4, 3)
            D2[c, at] = cut(f2 * frame_mask, xin) - 6.0 * inward(C0[c, at])

    kept_rows = (sub < 3) | (sub > 4)

    def aligned(first, last):
        return jnp.where(sub < 3, slide(last, 3), jnp.where(sub > 4, slide(first, 5), 0.0))

    def aligned_plane(S, c, i):
        return aligned(S[c, i, 0:8], S[c, i, Y - 8 : Y])

    seam = [up(frames[1]["f2", c] + aligned(strips[1][3][c][0], strips[1][3][c][last_tile]), 1) for c in range(comps)]
    for i in range(X):
        for c in range(comps):
            full = [
                aligned_plane(S0, c, i) + inward(C0[c, i]),
                aligned_plane(S1, c, i) + C1[c, i],
                aligned_plane(S2, c, i) + D2[c, i],
            ]
            f = full[2]
            fa = aligned_plane(S2, c, i + 1) + D2[c, i + 1]
            ya = jnp.where(sub == 7, slide(S2[c, i, 0:8], 4), slide(f, -1))
            ya = ya + jnp.where(sub == 0, slide(S2[c, i, Y - 8 : Y], 4), 0.0)
            za = jnp.where(lane == Z - 1, edge_of(seam[c], i), up(f, 1))
            full.append(fa + ya + za)
            kept = [[jnp.where(kept_rows, q, 0.0)] for q in full[:3]]
            add(c, [[q] for q in full], kept)

    line = jnp.zeros((8, Z), jnp.float32)
    for k, part in enumerate(sums):
        line = jnp.where(lane == k, jnp.sum(part, axis=1, keepdims=True), line)
    line = jnp.sum(line, axis=0, keepdims=True)

    if last_wave >= 2:
        heard(last_wave)

    def residual_basis():
        def spread(ts, f):
            ts = list(ts)
            ts[0] = ts[0] + jnp.where(sub < 3, slide(f, 3), 0.0)
            ts[last_tile] = ts[last_tile] + jnp.where(sub > 4, slide(f, 5), 0.0)
            return ts

        seam = [[None] * tiles for _ in range(comps)]
        for c in range(comps):
            ends_of = [spread(strips[side][3][c], frames[side]["f2", c]) for side in range(2)]
            seam[c] = [seam_of(ends_of[0][t], ends_of[1][t]) for t in range(tiles)]
        for at, after, before, xin in planes_of(1):
            for c in range(comps):
                ts = spread(split(S2[c, at]), D2[c, at])
                for t in range(tiles):
                    S2[c, at, 8 * t : 8 * t + 8] = ts[t]
        for i, after, before, xin in planes_of(0):
            for c in range(comps):
                B0[c, i] = joined(spread(split(S0[c, i]), inward(C0[c, i])))
                p1 = spread(split(S1[c, i]), C1[c, i])
                B1[c, i] = joined(p1)
                B2[c, i] = S2[c, i]
                beyond = slide(D2[c, i], 4)
                out = around_tiles(S2, seam, c, i, after, before, beyond, beyond)
                B3[c, i] = joined([out[t] - 9.0 * p1[t] for t in range(tiles)])

    order = 0
    for group, landing in zip(groups, gathered):
        mine = slot_of(sizes, group)
        row[...] = line
        landing[mine] = line
        offsets = [o for o in peers if o in offsets_of(sizes, group)]
        for moved in offsets:
            pltpu.make_async_remote_copy(
                src_ref=row, dst_ref=landing.at[mine], send_sem=gs.at[order], recv_sem=gr.at[order],
                device_id=around(sizes, moved), device_id_type=MESH_IDS,
            ).start()
        if order == 0:
            residual_basis()
        many = landing.at[pl.ds(0, len(offsets))]
        pltpu.make_async_copy(many, many, gr.at[order]).wait()
        line = landing[0]
        for k in range(1, len(offsets) + 1):
            line = line + landing[k]
        pltpu.make_async_copy(many, many, gs.at[order]).wait()
        order += 1

    own_diff.wait()
    for c in range(comps):
        g = {}
        for k, (a, b) in enumerate(PAIRS):
            at = k * comps + c
            g[a, b] = g[b, a] = jnp.broadcast_to(line[:, at : at + 1], (1, Z))
        g[2, 3] = g[3, 2] = 2.0 * g[2, 3] - 9.0 * g[1, 2]
        g[0, 3] = g[1, 2] - 9.0 * g[0, 1]
        g[1, 3] = g[2, 2] + 6.0 * g[0, 2] - 9.0 * g[1, 1]
        coef = jnp.full((1, Z), diff_ref[c], jnp.float32)
        diagonal = 1.0 + 6.0 * coef

        def image_of(d):
            return [
                diagonal * d[0] - 6.0 * coef * d[1],
                diagonal * d[1] - coef * (d[0] + 9.0 * d[2]),
                diagonal * d[2] - coef * d[1],
                -coef * d[2],
            ]

        def form(a, b):
            total = None
            for i, left in enumerate(a):
                for j, right in enumerate(b):
                    if left is zero or right is zero:
                        continue
                    term = left * right * g[i, j]
                    total = term if total is None else total + term
            return total

        zero = jnp.zeros((1, Z), jnp.float32)
        res = [zero + 1.0, zero, zero, zero]
        direction = [zero + 1.0, zero, zero]
        found = [zero, zero, zero]
        norm = g[0, 0]
        for iteration in range(3):
            image = image_of(direction)
            if iteration == 0:
                image = [image[0], image[1], zero, zero]
            elif iteration == 1:
                image = [image[0], image[1], image[2], zero]
            step = norm / form(direction, image)
            found = [f if d is zero else f + step * d for f, d in zip(found, direction)]
            res = [r if m is zero else r - step * m for r, m in zip(res, image)]
            if iteration < 2:
                after = form(res[:3], res[:3])
                ratio = after / norm
                direction = [r if d is zero else r + ratio * d for r, d in zip(res, direction)]
                norm = after
        for k, value in enumerate(found + res):
            co_ref[8 * c + k : 8 * c + k + 1] = value

    for copy, moved in copies:
        pl.when(exists(moved))(copy.wait_send)


def combine(co_ref, B0, B1, B2, B3, x_hbm, r_hbm, x_ref, r_ref, sems):
    comps, X, Y, Z = B0.shape
    copies = []
    for c in range(comps):
        f = [jnp.broadcast_to(co_ref[8 * c + k : 8 * c + k + 1], (Y, Z)) for k in range(7)]
        for x in range(X):
            p = [B[c, x] for B in (B0, B1, B2, B3)]
            x_ref[c, x] = f[0] * p[0] + f[1] * p[1] + f[2] * p[2]
            r_ref[c, x] = f[3] * p[0] + f[4] * p[1] + f[5] * p[2] + f[6] * p[3]
        for k, (src, dst) in enumerate(((x_ref, x_hbm), (r_ref, r_hbm))):
            copy = pltpu.make_async_copy(src.at[c], dst.at[c], sems.at[k, c])
            copy.start()
            copies.append(copy)
    for copy in copies:
        copy.wait()


def solution(mesh):
    sizes = tuple(mesh.shape[a] for a in AXES)
    groups = groups_of(sizes)

    def body(velocity, diffusion):
        comps, X, Y, Z = velocity.shape
        XR, YR = X + 2 * MARGIN, Y + 2 * MARGIN
        assert X == 2 * MARGIN and XR * 8 == Z and MARGIN * 2 == 8
        f32 = jnp.float32
        whole = pltpu.VMEM((comps, XR, YR, Z), f32)
        packed = pltpu.VMEM((comps, Y, Z), f32)
        inner = pltpu.VMEM((comps, XR, Y, Z), f32)
        frame = pltpu.VMEM((comps, XR, 8, Z), f32)
        strip = pltpu.VMEM((comps, YR, Z), f32)
        counts = [len(offsets_of(sizes, group)) + 1 for group in groups]
        out = pltpu.VMEM(velocity.shape, f32)
        vmem = pl.BlockSpec(memory_space=pltpu.VMEM)
        hbm = pl.BlockSpec(memory_space=pltpu.HBM)
        basis = pl.pallas_call(
            functools.partial(kernel, sizes),
            out_shape=(out, out, out, out, pltpu.VMEM((8 * comps, Z), f32)),
            in_specs=[hbm] * 2,
            out_specs=(vmem,) * 5,
            scratch_shapes=[
                pltpu.SMEM((comps,), f32),
                whole, inner, inner, inner,
                frame, frame, frame, frame, frame,
                packed, packed, packed, strip,
                pltpu.VMEM((2, Y, Z), f32), pltpu.VMEM((2, Y, Z), f32),
                pltpu.VMEM((2, YR, Z), f32), pltpu.VMEM((2, YR, Z), f32),
                pltpu.VMEM((8, Z), f32),
                pltpu.VMEM((8, Z), f32),
                pltpu.VMEM((1, Z), f32),
                *[pltpu.VMEM((count, 1, Z), f32) for count in counts],
                pltpu.SemaphoreType.DMA((16,)),
                pltpu.SemaphoreType.DMA((16,)),
                pltpu.SemaphoreType.DMA((len(groups),)),
                pltpu.SemaphoreType.DMA((len(groups),)),
                pltpu.SemaphoreType.DMA((2,)),
                pltpu.SemaphoreType.REGULAR((sizes[2] + 1, 2)),
            ],
            compiler_params=pltpu.CompilerParams(collective_id=0, has_side_effects=True, vmem_limit_bytes=GRANT),
        )(diffusion, velocity)
        shape = jax.ShapeDtypeStruct(velocity.shape, f32)
        return pl.pallas_call(
            combine,
            out_shape=(shape, shape),
            in_specs=[vmem] * 5,
            out_specs=(hbm, hbm),
            scratch_shapes=[
                pltpu.VMEM(velocity.shape, f32),
                pltpu.VMEM(velocity.shape, f32),
                pltpu.SemaphoreType.DMA((2, comps)),
            ],
            compiler_params=pltpu.CompilerParams(vmem_limit_bytes=SMALL),
        )(basis[4], *basis[:4])

    return jax.shard_map(
        body,
        mesh=mesh,
        in_specs=(P(None, "gx", "gy", "gz"), P()),
        out_specs=(P(None, "gx", "gy", "gz"), P(None, "gx", "gy", "gz")),
        check_vma=False,
    )
```

```python
import functools
import itertools

import jax
import jax.numpy as jnp
from jax import lax
from jax.experimental import pallas as pl
from jax.experimental.pallas import tpu as pltpu
from jax.sharding import PartitionSpec as P

AXES = ("gx", "gy", "gz")
MESH_IDS = pl.DeviceIdType.MESH
MARGIN = 4
PAIRS = ((0, 0), (0, 1), (1, 1), (0, 2), (1, 2), (2, 2), (2, 3))
time_step = 0.25
ONE_SHOT = 64
GRANT = 66200000
SMALL = 4194304
EARLY = False


def around(sizes, moved):
    return tuple(lax.rem(lax.axis_index(a) + o, s) for a, o, s in zip(AXES, moved, sizes))


def groups_of(sizes):
    total = sizes[0] * sizes[1] * sizes[2]
    if total <= ONE_SHOT:
        return [(0, 1, 2)]
    return [(0,), (1,), (2,)]


def offsets_of(sizes, group):
    ranges = [range(sizes[k]) if k in group else range(1) for k in range(3)]
    return [o for o in itertools.product(*ranges) if any(o)]


def slot_of(sizes, group):
    slot = 0
    for k in group:
        slot = slot * sizes[k] + lax.axis_index(AXES[k])
    return slot


def kernel(sizes, diff_hbm, v_hbm, B0, B1, B2, B3, co_ref, diff_ref, V, S0, S1, S2, D0, C0, D1, C1, D2, CC, YF, P1, P2, A0, A1, A2, YA, late, own, left_pack, right_pack, PX, WU, WD, low, high, mask_low, mask_high, row, *rest):
    groups = groups_of(sizes)
    gathered, (fs, fr, gs, gr, ins, waves) = rest[: len(groups)], rest[len(groups):]
    comps, X, Y, Z = v_hbm.shape
    M, D = MARGIN, MARGIN - 1
    XR, YR = X + 2 * M, Y + 2 * M
    tiles = Y // 8
    here = [lax.axis_index(a) for a in AXES]

    def exists(moved):
        ok = None
        for k in range(3):
            if moved[k]:
                place = here[k] + moved[k]
                one = (place >= 0) & (place < sizes[k])
                ok = one if ok is None else ok & one
        return ok

    def missing(moved):
        return pl.when(jnp.logical_not(exists(moved)))

    def shifted(moved):
        return tuple(h + m for h, m in zip(here, moved))

    peers = set()
    for group in groups:
        peers.update(offsets_of(sizes, group))
    for dx, dy in itertools.product((-1, 0, 1), (-1, 0, 1)):
        moved = (dx % sizes[0], dy % sizes[1], 0)
        if any(moved):
            peers.add(moved)
    peers = sorted(peers, key=lambda o: -sum(min(m, s - m) for m, s in zip(o, sizes)))
    barrier = pltpu.get_barrier_semaphore()
    relayed = len(groups) == 1
    greeted = [o for o in peers if not (relayed and o[2])]
    along_z = ((0, 0, -1), (0, 0, 1))
    last_wave = sizes[2] - 1 if relayed else 1

    own_cells = pltpu.make_async_copy(v_hbm, V.at[:, 0:X, 0:Y], ins.at[0])
    own_cells.start()
    own_diff = pltpu.make_async_copy(diff_hbm, diff_ref, ins.at[1])
    own_diff.start()

    expected = len(greeted)
    for moved in greeted:
        pl.semaphore_signal(barrier, inc=1, device_id=around(sizes, moved), device_id_type=MESH_IDS)
    for moved in along_z if relayed else ():
        @pl.when(exists(moved))
        def _(moved=moved):
            pl.semaphore_signal(barrier, inc=1, device_id=shifted(moved), device_id_type=MESH_IDS)

        expected = expected + exists(moved).astype(jnp.int32)

    def announce(wave):
        for k, moved in enumerate(along_z):
            @pl.when(exists(moved))
            def _(k=k, moved=moved):
                pl.semaphore_signal(waves.at[wave, k], inc=1, device_id=shifted(moved), device_id_type=MESH_IDS)

    def heard(wave):
        for k, moved in enumerate(along_z):
            @pl.when(exists(tuple(-m for m in moved)))
            def _(k=k):
                pl.semaphore_wait(waves.at[wave, k], 1)

    @missing((1, 0, 0))
    def _():
        V[:, X : X + M] = jnp.zeros((comps, M, YR, Z), jnp.float32)
        right_pack[...] = jnp.zeros((comps, Y, Z), jnp.float32)

    @missing((-1, 0, 0))
    def _():
        V[:, X + M : XR] = jnp.zeros((comps, M, YR, Z), jnp.float32)
        left_pack[...] = jnp.zeros((comps, Y, Z), jnp.float32)

    V[:, 0:X, Y + M : YR - D] = jnp.zeros((comps, X, 1, Z), jnp.float32)
    for ref in (low, high):
        ref[:, Y + D : YR - D] = jnp.zeros((2, 2, Z), jnp.float32)

    @missing((0, 1, 0))
    def _():
        V[:, 0:X, Y : Y + M] = jnp.zeros((comps, X, M, Z), jnp.float32)

    @missing((0, -1, 0))
    def _():
        V[:, 0:X, YR - D : YR] = jnp.zeros((comps, X, D, Z), jnp.float32)
        late[...] = jnp.zeros((comps, X, 1, Z), jnp.float32)

    for dz, ref in ((-1, low), (1, high)):
        @missing((0, 0, dz))
        def _(ref=ref):
            ref[:, 0:Y] = jnp.zeros((2, Y, Z), jnp.float32)

        for dy, first_row in ((1, Y), (-1, YR - D)):
            @missing((0, dy, dz))
            def _(ref=ref, first_row=first_row):
                ref[:, first_row : first_row + D] = jnp.zeros((2, D, Z), jnp.float32)

    lane = lax.broadcasted_iota(jnp.int32, (8, Z), 1)
    lanes = lax.broadcasted_iota(jnp.int32, (YR, Z), 1)
    k_low = lanes % 8 < M
    sub = lax.broadcasted_iota(jnp.int32, (8, Z), 0)
    xx = lane // 8
    xx = jnp.where(xx >= X + M, xx - XR, xx) + here[0] * X
    inside = (xx >= 0) & (xx < X * sizes[0])
    depth = lane % 8 - M
    mask_low[...] = jnp.where(inside & (depth + here[2] * Z >= 0), 1.0, 0.0).astype(jnp.float32)
    mask_high[...] = jnp.where(inside & (depth + here[2] * Z + Z < Z * sizes[2]), 1.0, 0.0).astype(jnp.float32)
    above = jnp.where(exists((0, 1, 0)), 1.0, 0.0).astype(jnp.float32)
    below = jnp.where(exists((0, -1, 0)), 1.0, 0.0).astype(jnp.float32)
    frame_mask = jnp.where(sub < M, above, below)
    one_sided = sizes[0] == 2
    for dx, ring_at in ((1, X), (-1, XR - 1)):
        @missing((dx, 0, 0))
        def _(ring_at=ring_at):
            for ref in (S0, S1, S2, C0, C1, D2):
                ref[:, ring_at] = jnp.zeros((comps,) + ref.shape[2:], jnp.float32)

    own_cells.wait()
    for c in range(comps):
        for t in range(tiles):
            packed = jnp.zeros((8, Z), jnp.float32)
            for x in range(X):
                rolled = pltpu.roll(V[c, x, 8 * t : 8 * t + 8], (8 * x + M) % Z, 1)
                packed = jnp.where(lane // 8 == x, rolled, packed)
            own[c, 8 * t : 8 * t + 8] = packed
    pl.semaphore_wait(barrier, expected)

    copies = []

    def plan(src, dst, moved):
        k = len(copies)
        copy = pltpu.make_async_remote_copy(
            src_ref=src, dst_ref=dst, send_sem=fs.at[k], recv_sem=fr.at[k],
            device_id=shifted(moved), device_id_type=MESH_IDS,
        )
        copies.append((copy, moved))
        return copy, moved

    def start(which, also=None):
        copy, moved = which
        ok = exists(moved)
        pl.when(ok if also is None else ok & also)(copy.start)

    def received(which):
        for copy, moved in which:
            pl.when(exists(tuple(-m for m in moved)))(copy.wait_recv)

    announce(1)
    x_packs = [plan(own, right_pack, (-1, 0, 0)), plan(own, left_pack, (1, 0, 0))]
    for which in x_packs:
        start(which)

    more = exists((1, 0, 0))
    begins = [jnp.where(more, X - M, 0), jnp.where(more, 0, X - M)]
    odd = lax.rem(here[1], 2) == 1
    y_faces = []
    for begin in begins:
        planes = pl.ds(begin, M)
        y_faces.append((
            plan(V.at[:, planes, 0:M], V.at[:, planes, Y : Y + M], (0, -1, 0)),
            plan(V.at[:, planes, Y - D : Y], V.at[:, planes, YR - D : YR], (0, 1, 0)),
        ))

    def start_far(pair):
        start(pair[1], odd)
        start(pair[0], jnp.logical_not(odd))

    def start_near(pair):
        start(pair[0], odd)
        start(pair[1], jnp.logical_not(odd))

    start_far(y_faces[0])
    start_near(y_faces[0])
    start_far(y_faces[1])
    x_faces = [
        plan(V.at[:, 0:M, 0:Y], V.at[:, X : X + M, 0:Y], (-1, 0, 0)),
        plan(V.at[:, X - M : X, 0:Y], V.at[:, X + M : XR, 0:Y], (1, 0, 0)),
    ]
    for which in x_faces:
        start(which)

    received(x_packs)
    for t in range(tiles):
        at = slice(8 * t, 8 * t + 8)
        px = []
        for c in range(comps):
            beside_x = jnp.where(lane < 8 * M, right_pack[c, at], left_pack[c, at])
            px.append(jnp.where(lane < 8 * X, own[c, at], pltpu.roll(beside_x, 8 * X, 1)))
            PX[c, at] = px[c]
        WU[0, at] = jnp.where(k_low[0:8], px[0], pltpu.roll(px[1], M, 1))
        WD[0, at] = jnp.where(k_low[0:8], pltpu.roll(px[1], Z - M, 1), px[0])
        WU[1, at] = px[2]
        WD[1, at] = px[2]
    z_edges, z_faces = [], []
    for dz, W, ref in ((-1, WD, high), (1, WU, low)):
        z_faces.append(plan(W, ref.at[:, 0:Y], (0, 0, dz)))
        start(z_faces[-1])
    heard(1)
    for dz, W, ref in ((-1, WD, high), (1, WU, low)):
        z_edges.append(plan(W.at[:, 0:D], ref.at[:, Y : Y + D], (0, -1, dz)))
        z_edges.append(plan(W.at[:, Y - D : Y], ref.at[:, YR - D : YR], (0, 1, dz)))
    for which in z_edges:
        start(which)
    start_near(y_faces[1])
    late_row = plan(V.at[:, 0:X, Y - M : Y - D], late, (0, 1, 0))
    start(late_row)
    if last_wave >= 2:
        announce(2)
    quarter = 0.5 * time_step
    low_lane = k_low[0:8]
    zero8 = jnp.zeros((8, Z), jnp.float32)

    def split(f):
        return [f[8 * t : 8 * t + 8] for t in range(tiles)]

    def joined(ts):
        return jnp.concatenate(ts, axis=0)

    def up(f, by):
        return pltpu.roll(f, Z - by, 1)

    def down(f, by):
        return pltpu.roll(f, by, 1)

    def slide(f, by):
        return pltpu.roll(f, by % 8, 0)

    def rows_after(ts, last=0.0):
        r = [slide(t, -1) for t in ts] + [last]
        return [jnp.where(sub == 7, r[t + 1], r[t]) for t in range(len(ts))]

    def rows_before(ts, first=0.0):
        r = [first] + [slide(t, 1) for t in ts]
        return [jnp.where(sub == 0, r[t], r[t + 1]) for t in range(len(ts))]

    def inward(f):
        f = jnp.where(sub < M, slide(f, 1), slide(f, -1))
        return jnp.where((sub == 0) | (sub == 7), 0.0, f)

    def edge_of(seam, at):
        return pltpu.roll(seam, (Z - M) - 8 * at, 1)

    def seam_of(low_field, high_field):
        return jnp.where(low_lane, up(high_field, 1), down(low_field, 1))

    def planes_of(reach):
        own_planes = [(i, (i + 1) % XR, (i - 1) % XR, None) for i in range(X)]
        outer = []
        for j in range(reach):
            if one_sided:
                outer.append((
                    jnp.where(more, X + j, XR - 1 - j),
                    jnp.where(more, X + j + 1, (XR - j) % XR),
                    jnp.where(more, X + j - 1, XR - 2 - j),
                    None,
                ))
            else:
                for i in (X + j, -1 - j):
                    place = here[0] * X + i
                    xin = jnp.where((place >= 0) & (place < X * sizes[0]), 1.0, 0.0).astype(jnp.float32)
                    outer.append((i % XR, (i + 1) % XR, (i - 1) % XR, xin))
        return own_planes + outer

    def cut(value, xin):
        return value if xin is None else value * xin

    received(x_faces)
    for at, after, before, xin in planes_of(D):
        v = [split(V[c, at, 0:Y]) for c in range(comps)]
        va = [split(V[c, after, 0:Y]) for c in range(comps)]
        vb = [split(V[c, before, 0:Y]) for c in range(comps)]
        for c in range(comps):
            fy = [v[1][t] * v[c][t] for t in range(tiles)]
            ya, yb = rows_after(fy), rows_before(fy)
            YF[c, at] = jnp.where(sub == 7, slide(fy[0], -1), slide(fy[-1], 1))
            for t in range(tiles):
                fz = v[2][t] * v[c][t]
                total = va[0][t] * va[c][t] - vb[0][t] * vb[c][t]
                total = total + (ya[t] - yb[t])
                za = jnp.where(lane == Z - 1, 0.0, up(fz, 1))
                zb = jnp.where(lane == 0, 0.0, down(fz, 1))
                total = total + (za - zb)
                S0[c, at, 8 * t : 8 * t + 8] = cut(v[c][t] - quarter * total, xin)

    for wave in range(2, last_wave):
        heard(wave)
        announce(wave + 1)

    forwards = [
        plan(V.at[:, 0:M, Y:YR], V.at[:, X : X + M, Y:YR], (-1, 0, 0)),
        plan(V.at[:, X - M : X, Y:YR], V.at[:, X + M : XR, Y:YR], (1, 0, 0)),
    ]
    received(y_faces[0])
    start(forwards[1])
    start(forwards[0], jnp.logical_not(more))
    received(z_faces)

    masks = [mask_low[...], mask_high[...]]
    strip_v = [[], []]
    for t in range(tiles):
        at = slice(8 * t, 8 * t + 8)
        outer = (low[0, at], up(low[0, at], M), low[1, at])
        strip_v[0].append([jnp.where(low_lane, outer[c], PX[c, at]) for c in range(comps)])
        outer = (high[0, at], down(high[0, at], M), high[1, at])
        strip_v[1].append([jnp.where(low_lane, PX[c, at], outer[c]) for c in range(comps)])
    strips = [[[None] * comps for _ in range(4)] for _ in range(2)]
    for side in range(2):
        v = strip_v[side]
        inner = masks[side]
        for c in range(comps):
            fy = [v[t][1] * v[t][c] for t in range(tiles)]
            ya, yb = rows_after(fy), rows_before(fy)
            fields = [[], []]
            for t in range(tiles):
                fx, fz = v[t][0] * v[t][c], v[t][2] * v[t][c]
                total = up(fx, 8) - down(fx, 8)
                total = total + (ya[t] - yb[t])
                total = total + (up(fz, 1) - down(fz, 1))
                fields[0].append(fz)
                fields[1].append((v[t][c] - quarter * total) * inner)
            strips[side][0][c], strips[side][1][c] = fields
        for k in (2, 3):
            for c in range(comps):
                f = strips[side][k - 1][c]
                ya, yb = rows_after(f), rows_before(f)
                out = []
                for t in range(tiles):
                    total = (up(f[t], 8) + down(f[t], 8)) + (ya[t] + yb[t]) + (up(f[t], 1) + down(f[t], 1))
                    total = total * inner
                    out.append(total if k == 2 else total - 6.0 * strips[side][1][c][t])
                strips[side][k][c] = out

    def seams_of(k):
        return [[seam_of(strips[0][k][c][t], strips[1][k][c][t]) for t in range(tiles)] for c in range(comps)]

    flip = jnp.where(lane % 8 < M, quarter, -quarter)
    border = (lane == 0) | (lane == Z - 1)
    seam = [[s * flip for s in ts] for ts in seams_of(0)]
    for at, after, before, xin in planes_of(D):
        for c in range(comps):
            for t in range(tiles):
                edge = cut(edge_of(seam[c][t], at), xin)
                rows = slice(8 * t, 8 * t + 8)
                S0[c, at, rows] = S0[c, at, rows] - jnp.where(border, edge, 0.0)

    def around_tiles(ref, seam, c, at, after, before, first=0.0, last=0.0):
        f = split(ref[c, at])
        fa, fb = split(ref[c, after]), split(ref[c, before])
        ya, yb = rows_after(f, last), rows_before(f, first)
        out = []
        for t in range(tiles):
            edge = edge_of(seam[c][t], at)
            za = jnp.where(lane == Z - 1, edge, up(f[t], 1))
            zb = jnp.where(lane == 0, edge, down(f[t], 1))
            out.append((fa[t] + fb[t]) + (ya[t] + yb[t]) + (za + zb))
        return out

    seam = seams_of(1)
    for at, after, before, xin in planes_of(2):
        for c in range(comps):
            out = around_tiles(S0, seam, c, at, after, before)
            for t in range(tiles):
                S1[c, at, 8 * t : 8 * t + 8] = cut(out[t], xin)
    seam = seams_of(2)
    for at, after, before, xin in planes_of(1):
        for c in range(comps):
            out = around_tiles(S1, seam, c, at, after, before)
            for t in range(tiles):
                rows = slice(8 * t, 8 * t + 8)
                S2[c, at, rows] = cut(out[t], xin) - 6.0 * S0[c, at, rows]

    def from_tiles(first, last, by_first, by_last, at_first, at_last):
        return jnp.where(sub == at_last, slide(last, by_last), jnp.where(sub == at_first, slide(first, by_first), 0.0))

    def aligned(first, last):
        return jnp.where(sub < 3, slide(last, 3), jnp.where(sub > 4, slide(first, 5), 0.0))

    for at, after, before, xin in planes_of(2):
        for c in range(comps):
            P1[c, at] = cut(from_tiles(S0[c, at, 0:8], S0[c, at, Y - 8 : Y], 5, 3, 5, 2), xin)
    for at, after, before, xin in planes_of(1):
        for c in range(comps):
            P2[c, at] = cut(from_tiles(S1[c, at, 0:8], S1[c, at, Y - 8 : Y], 4, 4, 4, 3), xin)
    for i in range(X + 1):
        for c in range(comps):
            first, last = S2[c, i, 0:8], S2[c, i, Y - 8 : Y]
            A2[c, i] = aligned(first, last)
            if i < X:
                A0[c, i] = aligned(S0[c, i, 0:8], S0[c, i, Y - 8 : Y])
                A1[c, i] = aligned(S1[c, i, 0:8], S1[c, i, Y - 8 : Y])
                YA[c, i] = jnp.where((sub == 0) | (sub == 7), jnp.where(sub == 7, slide(first, 4), slide(last, 4)), 0.0)

    sums = [None] * (len(PAIRS) * comps)

    def add(c, full, kept):
        for k, (a, b) in enumerate(PAIRS):
            part = None
            for left, right in zip(kept[a], full[b]):
                part = left * right if part is None else part + left * right
            at = k * comps + c
            sums[at] = part if sums[at] is None else sums[at] + part

    crossing = (lane % 8 == M - 1) & (lane < 8 * X)
    last_tile = tiles - 1
    for i in range(X):
        for c in range(comps):
            full = [split(S[c, i]) for S in (S0, S1, S2)]
            f = full[2]
            fa = split(S2[c, i + 1])
            ya = rows_after(f)
            ya[last_tile] = jnp.where(sub < 4, ya[last_tile], 0.0)
            out = []
            for t in range(tiles):
                za = jnp.where(lane == Z - 1, 0.0, up(f[t], 1))
                out.append(fa[t] + ya[t] + za)
            kept = []
            for a in range(3):
                ts = list(full[a])
                ts[0] = jnp.where(sub >= 3, ts[0], 0.0)
                ts[last_tile] = jnp.where(sub < 5, ts[last_tile], 0.0)
                kept.append(ts)
            add(c, full + [out], kept)
            if i == 0:
                at = (len(PAIRS) - 1) * comps + c
                for t in range(tiles):
                    f = strips[1][3][c][t]
                    f = jnp.where(sub >= 3, f, 0.0) if t == 0 else f
                    f = jnp.where(sub < 5, f, 0.0) if t == last_tile else f
                    sums[at] = sums[at] + jnp.where(crossing, f * up(f, 1), 0.0)

    received(y_faces[1])
    start(forwards[0], more)
    received(forwards)
    received(z_edges)
    packed2 = []
    for c in range(comps):
        packed = zero8
        for x in range(XR):
            rolled = pltpu.roll(V[c, x, Y:YR], (8 * x + M) % Z, 1)
            packed = jnp.where(lane // 8 == x, rolled, packed)
        packed2.append(packed)

    ends = (sub == 0) | (sub == 7)
    signed = jnp.where(sub == 0, -quarter, quarter)

    def frame_of(center, corr):
        f = jnp.where(sub < M, slide(center, 1), slide(center, -1))
        return jnp.where(ends, corr, f)

    def frame_section(v2, end, c, fx_part, z_part, inner):
        fy2 = v2[1] * v2[c]
        ya = jnp.where(sub == 7, end, slide(fy2, -1))
        yb = jnp.where(sub == 0, end, slide(fy2, 1))
        value = (v2[c] - quarter * (fx_part + (ya - yb) + z_part)) * inner
        return frame_of(value, signed * fy2)

    at = slice(Y, YR)
    outer = (low[0, at], up(low[0, at], M), low[1, at])
    strip_v[0].append([jnp.where(low_lane, outer[c], packed2[c]) for c in range(comps)])
    outer = (high[0, at], down(high[0, at], M), high[1, at])
    strip_v[1].append([jnp.where(low_lane, packed2[c], outer[c]) for c in range(comps)])
    frames = [dict() for _ in range(2)]
    for side in range(2):
        v = strip_v[side]
        inner = masks[side] * frame_mask
        for c in range(comps):
            v2 = v[tiles]
            fx, fz = v2[0] * v2[c], v2[2] * v2[c]
            frames[side]["fz", c] = fz
            end = jnp.where(sub == 7, slide(v[0][1] * v[0][c], -1), slide(v[last_tile][1] * v[last_tile][c], 1))
            f0 = frame_section(v2, end, c, up(fx, 8) - down(fx, 8), up(fz, 1) - down(fz, 1), inner)
            f0 = jnp.where(ends, f0 * masks[side], f0)
            c0 = inward(f0)
            s = strips[side]
            f1 = (up(c0, 8) + down(c0, 8)) + (up(c0, 1) + down(c0, 1)) + f0 + inward(c0)
            f1 = (f1 + from_tiles(s[1][c][0], s[1][c][last_tile], 5, 3, 5, 2)) * inner
            c1 = inward(f1)
            f2 = (up(c1, 8) + down(c1, 8)) + (up(c1, 1) + down(c1, 1)) + f1 + inward(c1)
            f2 = (f2 + from_tiles(s[2][c][0], s[2][c][last_tile], 4, 4, 4, 3)) * inner - 6.0 * inward(c0)
            frames[side]["c0", c], frames[side]["c1", c], frames[side]["f2", c] = c0, c1, f2

    def frame_seam(name, c):
        return seam_of(frames[0][name, c], frames[1][name, c])

    seam = [frame_seam("fz", c) for c in range(comps)]
    for at, after, before, xin in planes_of(D):
        v2 = [V[c, at, Y:YR] for c in range(comps)]
        va = [V[c, after, Y:YR] for c in range(comps)]
        vb = [V[c, before, Y:YR] for c in range(comps)]
        for c in range(comps):
            fz = v2[2] * v2[c]
            edge = edge_of(seam[c], at)
            z_part = jnp.where(lane == Z - 1, edge, up(fz, 1)) - jnp.where(lane == 0, edge, down(fz, 1))
            f0 = frame_section(v2, YF[c, at], c, va[0] * va[c] - vb[0] * vb[c], z_part, frame_mask)
            f0 = cut(f0, xin)
            D0[c, at] = f0
            C0[c, at] = inward(f0)

    def around_frame(C, seam, c, at, after, before):
        f = C[c, at]
        edge = edge_of(seam[c], at)
        za = jnp.where(lane == Z - 1, edge, up(f, 1))
        zb = jnp.where(lane == 0, edge, down(f, 1))
        return (C[c, after] + C[c, before]) + (za + zb), inward(f)

    seam = [frame_seam("c0", c) for c in range(comps)]
    for at, after, before, xin in planes_of(2):
        for c in range(comps):
            f1, twice = around_frame(C0, seam, c, at, after, before)
            CC[c, at] = twice
            f1 = (cut(f1 + (twice + D0[c, at]), xin) + P1[c, at]) * frame_mask
            D1[c, at] = f1
            C1[c, at] = inward(f1)
    seam = [frame_seam("c1", c) for c in range(comps)]
    for at, after, before, xin in planes_of(1):
        for c in range(comps):
            f2, twice = around_frame(C1, seam, c, at, after, before)
            f2 = f2 + (twice + D1[c, at])
            D2[c, at] = (cut(f2, xin) + P2[c, at]) * frame_mask - 6.0 * CC[c, at]

    kept_rows = (sub < 3) | (sub > 4)

    for c in range(comps):
        f = frames[1]["f2", c] + aligned(strips[1][3][c][0], strips[1][3][c][last_tile])
        at = (len(PAIRS) - 1) * comps + c
        sums[at] = sums[at] + jnp.where(crossing & kept_rows, f * up(f, 1), 0.0)
    for i in range(X):
        for c in range(comps):
            full = [
                A0[c, i] + CC[c, i],
                A1[c, i] + C1[c, i],
                A2[c, i] + D2[c, i],
            ]
            f = full[2]
            fa = A2[c, i + 1] + D2[c, i + 1]
            ya = jnp.where(sub == 7, 0.0, slide(f, -1)) + YA[c, i]
            za = jnp.where(lane == Z - 1, 0.0, up(f, 1))
            full.append(fa + ya + za)
            kept = [[jnp.where(kept_rows, q, 0.0)] for q in full[:3]]
            add(c, [[q] for q in full], kept)

    line = jnp.zeros((8, Z), jnp.float32)
    several = [line] * 4
    for k, part in enumerate(sums):
        several[k % 4] = jnp.where(lane == k, jnp.sum(part, axis=1, keepdims=True), several[k % 4])
    line = (several[0] + several[1]) + (several[2] + several[3])
    line = jnp.sum(line, axis=0, keepdims=True)

    if last_wave >= 2:
        heard(last_wave)

    def residual_basis():
        received([late_row])

        def spread(ts, f):
            ts = list(ts)
            ts[0] = ts[0] + jnp.where(sub < 3, slide(f, 3), 0.0)
            ts[last_tile] = ts[last_tile] + jnp.where(sub > 4, slide(f, 5), 0.0)
            return ts

        seam = [[None] * tiles for _ in range(comps)]
        for c in range(comps):
            ends_of = [spread(strips[side][3][c], frames[side]["f2", c]) for side in range(2)]
            seam[c] = [seam_of(ends_of[0][t], ends_of[1][t]) for t in range(tiles)]
        for at, after, before, xin in planes_of(1):
            for c in range(comps):
                ts = spread(split(S2[c, at]), D2[c, at])
                for t in range(tiles):
                    S2[c, at, 8 * t : 8 * t + 8] = ts[t]
        for i, after, before, xin in planes_of(0):
            for c in range(comps):
                B0[c, i] = joined(spread(split(S0[c, i]), CC[c, i]))
                p1 = spread(split(S1[c, i]), C1[c, i])
                B1[c, i] = joined(p1)
                B2[c, i] = S2[c, i]
                beyond = slide(D2[c, i], 4)
                out = around_tiles(S2, seam, c, i, after, before, beyond, beyond)
                far = jnp.broadcast_to(quarter * (late[1, i] * late[c, i]), (8, Z))
                out[0] = out[0] + jnp.where(sub == 0, far, 0.0)
                B3[c, i] = joined([out[t] - 9.0 * p1[t] for t in range(tiles)])

    def added(terms):
        while len(terms) > 1:
            terms = [terms[k] + terms[k + 1] if k + 1 < len(terms) else terms[k] for k in range(0, len(terms), 2)]
        return terms[0]

    own_diff.wait()
    order = 0
    for group, landing in zip(groups, gathered):
        mine = slot_of(sizes, group)
        row[...] = line
        landing[mine] = line
        offsets = [o for o in peers if o in offsets_of(sizes, group)]
        for moved in offsets:
            pltpu.make_async_remote_copy(
                src_ref=row, dst_ref=landing.at[mine], send_sem=gs.at[order], recv_sem=gr.at[order],
                device_id=around(sizes, moved), device_id_type=MESH_IDS,
            ).start()
        if order == 0:
            residual_basis()
        many = landing.at[pl.ds(0, len(offsets))]
        pltpu.make_async_copy(many, many, gr.at[order]).wait()
        line = added([landing[k] for k in range(len(offsets) + 1)])
        pltpu.make_async_copy(many, many, gs.at[order]).wait()
        order += 1

    for c in range(comps):
        g = {}
        for k, (a, b) in enumerate(PAIRS):
            at = k * comps + c
            g[a, b] = g[b, a] = jnp.broadcast_to(line[:, at : at + 1], (1, Z))
        g[2, 3] = g[3, 2] = 2.0 * g[2, 3] - 9.0 * g[1, 2]
        g[0, 3] = g[1, 2] - 9.0 * g[0, 1]
        g[1, 3] = g[2, 2] + 6.0 * g[0, 2] - 9.0 * g[1, 1]
        coef = jnp.full((1, Z), diff_ref[c], jnp.float32)
        diagonal = 1.0 + 6.0 * coef

        def image_of(d):
            return [
                diagonal * d[0] - 6.0 * coef * d[1],
                diagonal * d[1] - coef * (d[0] + 9.0 * d[2]),
                diagonal * d[2] - coef * d[1],
                -coef * d[2],
            ]

        def form(a, b):
            terms = []
            for i, left in enumerate(a):
                inside = [right * g[i, j] for j, right in enumerate(b) if right is not zero]
                if left is not zero:
                    terms.append(left * added(inside))
            return added(terms)

        zero = jnp.zeros((1, Z), jnp.float32)
        res = [zero + 1.0, zero, zero, zero]
        direction = [zero + 1.0, zero, zero]
        found = [zero, zero, zero]
        norm = g[0, 0]
        inverse = 1.0 / norm
        for iteration in range(3):
            image = image_of(direction)
            if iteration == 0:
                image = [image[0], image[1], zero, zero]
            elif iteration == 1:
                image = [image[0], image[1], image[2], zero]
            step = norm / form(direction, image)
            found = [f if d is zero else f + step * d for f, d in zip(found, direction)]
            res = [r if m is zero else r - step * m for r, m in zip(res, image)]
            if iteration < 2:
                after = form(res[:3], res[:3])
                ratio = after * inverse
                inverse = 1.0 / after
                direction = [r if d is zero else r + ratio * d for r, d in zip(res, direction)]
                norm = after
        for k, value in enumerate(found + res):
            co_ref[8 * c + k : 8 * c + k + 1] = value

    for copy, moved in copies:
        pl.when(exists(moved))(copy.wait_send)


def combine(co_ref, B0, B1, B2, B3, x_hbm, r_hbm, x_ref, r_ref, sems):
    comps, X, Y, Z = B0.shape
    copies = []
    for c in range(comps):
        f = [jnp.broadcast_to(co_ref[8 * c + k : 8 * c + k + 1], (Y, Z)) for k in range(7)]
        for x in range(X):
            p = [B[c, x] for B in (B0, B1, B2, B3)]
            x_ref[c, x] = f[0] * p[0] + f[1] * p[1] + f[2] * p[2]
            r_ref[c, x] = f[3] * p[0] + f[4] * p[1] + f[5] * p[2] + f[6] * p[3]
        for k, (src, dst) in enumerate(((x_ref, x_hbm), (r_ref, r_hbm))):
            copy = pltpu.make_async_copy(src.at[c], dst.at[c], sems.at[k, c])
            copy.start()
            copies.append(copy)
    for copy in copies:
        copy.wait()


def solution(mesh):
    sizes = tuple(mesh.shape[a] for a in AXES)
    groups = groups_of(sizes)

    def body(velocity, diffusion):
        comps, X, Y, Z = velocity.shape
        XR, YR = X + 2 * MARGIN, Y + 2 * MARGIN
        assert X == 2 * MARGIN and XR * 8 == Z and MARGIN * 2 == 8
        f32 = jnp.float32
        whole = pltpu.VMEM((comps, XR, YR, Z), f32)
        packed = pltpu.VMEM((comps, Y, Z), f32)
        inner = pltpu.VMEM((comps, XR, Y, Z), f32)
        frame = pltpu.VMEM((comps, XR, 8, Z), f32)
        strip = pltpu.VMEM((comps, YR, Z), f32)
        counts = [len(offsets_of(sizes, group)) + 1 for group in groups]
        out = pltpu.VMEM(velocity.shape, f32)
        vmem = pl.BlockSpec(memory_space=pltpu.VMEM)
        hbm = pl.BlockSpec(memory_space=pltpu.HBM)
        basis = pl.pallas_call(
            functools.partial(kernel, sizes),
            out_shape=(out, out, out, out, pltpu.VMEM((8 * comps, Z), f32)),
            in_specs=[hbm] * 2,
            out_specs=(vmem,) * 5,
            scratch_shapes=[
                pltpu.SMEM((comps,), f32),
                whole, inner, inner, inner,
                *[frame] * 13,
                pltpu.VMEM((comps, X, 1, Z), f32),
                packed, packed, packed, strip,
                pltpu.VMEM((2, Y, Z), f32), pltpu.VMEM((2, Y, Z), f32),
                pltpu.VMEM((2, YR, Z), f32), pltpu.VMEM((2, YR, Z), f32),
                pltpu.VMEM((8, Z), f32),
                pltpu.VMEM((8, Z), f32),
                pltpu.VMEM((1, Z), f32),
                *[pltpu.VMEM((count, 1, Z), f32) for count in counts],
                pltpu.SemaphoreType.DMA((17,)),
                pltpu.SemaphoreType.DMA((17,)),
                pltpu.SemaphoreType.DMA((len(groups),)),
                pltpu.SemaphoreType.DMA((len(groups),)),
                pltpu.SemaphoreType.DMA((2,)),
                pltpu.SemaphoreType.REGULAR((sizes[2] + 1, 2)),
            ],
            compiler_params=pltpu.CompilerParams(collective_id=0, has_side_effects=True, vmem_limit_bytes=GRANT),
        )(diffusion, velocity)
        shape = jax.ShapeDtypeStruct(velocity.shape, f32)
        return pl.pallas_call(
            combine,
            out_shape=(shape, shape),
            in_specs=[vmem] * 5,
            out_specs=(hbm, hbm),
            scratch_shapes=[
                pltpu.VMEM(velocity.shape, f32),
                pltpu.VMEM(velocity.shape, f32),
                pltpu.SemaphoreType.DMA((2, comps)),
            ],
            compiler_params=pltpu.CompilerParams(vmem_limit_bytes=SMALL),
        )(basis[4], *basis[:4])

    return jax.shard_map(
        body,
        mesh=mesh,
        in_specs=(P(None, "gx", "gy", "gz"), P()),
        out_specs=(P(None, "gx", "gy", "gz"), P(None, "gx", "gy", "gz")),
        check_vma=False,
    )
```

```python
import functools
import itertools

import jax
import jax.numpy as jnp
from jax import lax
from jax.experimental import pallas as pl
from jax.experimental.pallas import tpu as pltpu
from jax.sharding import PartitionSpec as P

AXES = ("gx", "gy", "gz")
MESH_IDS = pl.DeviceIdType.MESH
MARGIN = 4
PAIRS = ((0, 0), (0, 1), (1, 1), (0, 2), (1, 2), (2, 2), (2, 3))
time_step = 0.25
ONE_SHOT = 64
GRANT = 66200000
SMALL = 4194304
EARLY = False


def around(sizes, moved):
    return tuple(lax.rem(lax.axis_index(a) + o, s) for a, o, s in zip(AXES, moved, sizes))


def groups_of(sizes):
    total = sizes[0] * sizes[1] * sizes[2]
    if total <= ONE_SHOT:
        return [(0, 1, 2)]
    return [(0,), (1,), (2,)]


def offsets_of(sizes, group):
    ranges = [range(sizes[k]) if k in group else range(1) for k in range(3)]
    return [o for o in itertools.product(*ranges) if any(o)]


def slot_of(sizes, group):
    slot = 0
    for k in group:
        slot = slot * sizes[k] + lax.axis_index(AXES[k])
    return slot


def kernel(sizes, diff_hbm, v_hbm, B0, B1, B2, B3, co_ref, diff_ref, V, S0, S1, S2, D0, C0, D1, C1, D2, CC, YF, P1, P2, A0, A1, A2, YA, late, own, turned, left_pack, right_pack, PX, WU, WD, low, high, mask_low, mask_high, row, *rest):
    groups = groups_of(sizes)
    gathered, (fs, fr, gs, gr, ins, waves) = rest[: len(groups)], rest[len(groups):]
    comps, X, Y, Z = v_hbm.shape
    M, D = MARGIN, MARGIN - 1
    XR, YR = X + 2 * M, Y + 2 * M
    tiles = Y // 8
    here = [lax.axis_index(a) for a in AXES]

    def exists(moved):
        ok = None
        for k in range(3):
            if moved[k]:
                place = here[k] + moved[k]
                one = (place >= 0) & (place < sizes[k])
                ok = one if ok is None else ok & one
        return ok

    def missing(moved):
        return pl.when(jnp.logical_not(exists(moved)))

    def shifted(moved):
        return tuple(h + m for h, m in zip(here, moved))

    peers = set()
    for group in groups:
        peers.update(offsets_of(sizes, group))
    for dx, dy in itertools.product((-1, 0, 1), (-1, 0, 1)):
        moved = (dx % sizes[0], dy % sizes[1], 0)
        if any(moved):
            peers.add(moved)
    peers = sorted(peers, key=lambda o: -sum(min(m, s - m) for m, s in zip(o, sizes)))
    barrier = pltpu.get_barrier_semaphore()
    relayed = len(groups) == 1
    greeted = [o for o in peers if not (relayed and o[2])]
    along_z = ((0, 0, -1), (0, 0, 1))
    last_wave = sizes[2] - 1 if relayed else 1

    own_cells = pltpu.make_async_copy(v_hbm, V.at[:, 0:X, 0:Y], ins.at[0])
    own_cells.start()
    own_diff = pltpu.make_async_copy(diff_hbm, diff_ref, ins.at[1])
    own_diff.start()

    expected = len(greeted)
    for moved in greeted:
        pl.semaphore_signal(barrier, inc=1, device_id=around(sizes, moved), device_id_type=MESH_IDS)
    for moved in along_z if relayed else ():
        @pl.when(exists(moved))
        def _(moved=moved):
            pl.semaphore_signal(barrier, inc=1, device_id=shifted(moved), device_id_type=MESH_IDS)

        expected = expected + exists(moved).astype(jnp.int32)

    def announce(wave):
        for k, moved in enumerate(along_z):
            @pl.when(exists(moved))
            def _(k=k, moved=moved):
                pl.semaphore_signal(waves.at[wave, k], inc=1, device_id=shifted(moved), device_id_type=MESH_IDS)

    def heard(wave):
        for k, moved in enumerate(along_z):
            @pl.when(exists(tuple(-m for m in moved)))
            def _(k=k):
                pl.semaphore_wait(waves.at[wave, k], 1)

    @missing((1, 0, 0))
    def _():
        V[:, X : X + M] = jnp.zeros((comps, M, YR, Z), jnp.float32)
        right_pack[...] = jnp.zeros((comps + 2, Y, Z), jnp.float32)

    @missing((-1, 0, 0))
    def _():
        V[:, X + M : XR] = jnp.zeros((comps, M, YR, Z), jnp.float32)
        left_pack[...] = jnp.zeros((comps + 2, Y, Z), jnp.float32)

    V[:, 0:X, Y + M : YR - D] = jnp.zeros((comps, X, 1, Z), jnp.float32)
    for ref in (low, high):
        ref[:, Y + D : YR - D] = jnp.zeros((2, 2, Z), jnp.float32)

    @missing((0, 1, 0))
    def _():
        V[:, 0:X, Y : Y + M] = jnp.zeros((comps, X, M, Z), jnp.float32)

    @missing((0, -1, 0))
    def _():
        V[:, 0:X, YR - D : YR] = jnp.zeros((comps, X, D, Z), jnp.float32)
        late[...] = jnp.zeros((comps, X, 1, Z), jnp.float32)

    for dz, ref in ((-1, low), (1, high)):
        @missing((0, 0, dz))
        def _(ref=ref):
            ref[:, 0:Y] = jnp.zeros((2, Y, Z), jnp.float32)

        for dy, first_row in ((1, Y), (-1, YR - D)):
            @missing((0, dy, dz))
            def _(ref=ref, first_row=first_row):
                ref[:, first_row : first_row + D] = jnp.zeros((2, D, Z), jnp.float32)

    lane = lax.broadcasted_iota(jnp.int32, (8, Z), 1)
    lanes = lax.broadcasted_iota(jnp.int32, (YR, Z), 1)
    low_lane = lane % 8 < M
    sub = lax.broadcasted_iota(jnp.int32, (8, Z), 0)
    xx = lane // 8
    xx = jnp.where(xx >= X + M, xx - XR, xx) + here[0] * X
    inside = (xx >= 0) & (xx < X * sizes[0])
    depth = lane % 8 - M
    mask_low[...] = jnp.where(inside & (depth + here[2] * Z >= 0), 1.0, 0.0).astype(jnp.float32)
    mask_high[...] = jnp.where(inside & (depth + here[2] * Z + Z < Z * sizes[2]), 1.0, 0.0).astype(jnp.float32)
    above = jnp.where(exists((0, 1, 0)), 1.0, 0.0).astype(jnp.float32)
    below = jnp.where(exists((0, -1, 0)), 1.0, 0.0).astype(jnp.float32)
    frame_mask = jnp.where(sub < M, above, below)
    one_sided = sizes[0] == 2
    for dx, ring_at in ((1, X), (-1, XR - 1)):
        @missing((dx, 0, 0))
        def _(ring_at=ring_at):
            for ref in (S0, S1, S2, C0, C1, D2):
                ref[:, ring_at] = jnp.zeros((comps,) + ref.shape[2:], jnp.float32)

    own_cells.wait()
    for c in range(comps):
        for t in range(tiles):
            packed = jnp.zeros((8, Z), jnp.float32)
            for x in range(X):
                rolled = pltpu.roll(V[c, x, 8 * t : 8 * t + 8], (8 * x + M) % Z, 1)
                packed = jnp.where(lane // 8 == x, rolled, packed)
            at = slice(8 * t, 8 * t + 8)
            own[c, at] = packed
            turned[c, at] = pltpu.roll(packed, 8 * X, 1)
            if c == 1:
                own[comps, at] = pltpu.roll(packed, M, 1)
                own[comps + 1, at] = pltpu.roll(packed, Z - M, 1)
                turned[comps, at] = pltpu.roll(packed, 8 * X + M, 1)
                turned[comps + 1, at] = pltpu.roll(packed, 8 * X - M, 1)
    pl.semaphore_wait(barrier, expected)

    copies = []

    def plan(src, dst, moved):
        k = len(copies)
        copy = pltpu.make_async_remote_copy(
            src_ref=src, dst_ref=dst, send_sem=fs.at[k], recv_sem=fr.at[k],
            device_id=shifted(moved), device_id_type=MESH_IDS,
        )
        copies.append((copy, moved))
        return copy, moved

    def start(which, also=None):
        copy, moved = which
        ok = exists(moved)
        pl.when(ok if also is None else ok & also)(copy.start)

    def received(which):
        for copy, moved in which:
            pl.when(exists(tuple(-m for m in moved)))(copy.wait_recv)

    announce(1)
    x_packs = [plan(turned, right_pack, (-1, 0, 0)), plan(turned, left_pack, (1, 0, 0))]
    for which in x_packs:
        start(which)

    more = exists((1, 0, 0))
    begins = [jnp.where(more, X - M, 0), jnp.where(more, 0, X - M)]
    odd = lax.rem(here[1], 2) == 1
    y_faces = []
    for begin in begins:
        planes = pl.ds(begin, M)
        y_faces.append((
            plan(V.at[:, planes, 0:M], V.at[:, planes, Y : Y + M], (0, -1, 0)),
            plan(V.at[:, planes, Y - D : Y], V.at[:, planes, YR - D : YR], (0, 1, 0)),
        ))

    def start_far(pair):
        start(pair[1], odd)
        start(pair[0], jnp.logical_not(odd))

    def start_near(pair):
        start(pair[0], odd)
        start(pair[1], jnp.logical_not(odd))

    start_far(y_faces[0])
    start_near(y_faces[0])
    start_far(y_faces[1])
    x_faces = [
        plan(V.at[:, 0:M, 0:Y], V.at[:, X : X + M, 0:Y], (-1, 0, 0)),
        plan(V.at[:, X - M : X, 0:Y], V.at[:, X + M : XR, 0:Y], (1, 0, 0)),
    ]
    for which in x_faces:
        start(which)

    received(x_packs)
    for t in range(tiles):
        at = slice(8 * t, 8 * t + 8)
        px = []
        for k in range(comps + 2):
            beside_x = jnp.where(lane < 8 * (X + M), right_pack[k, at], left_pack[k, at])
            px.append(jnp.where(lane < 8 * X, own[k, at], beside_x))
        for c in range(comps):
            PX[c, at] = px[c]
        WU[0, at] = jnp.where(low_lane, px[0], px[comps])
        WD[0, at] = jnp.where(low_lane, px[comps + 1], px[0])
        WU[1, at] = px[2]
        WD[1, at] = px[2]
    z_edges, z_faces = [], []
    for dz, W, ref in ((-1, WD, high), (1, WU, low)):
        z_faces.append(plan(W, ref.at[:, 0:Y], (0, 0, dz)))
        start(z_faces[-1])
    heard(1)
    for dz, W, ref in ((-1, WD, high), (1, WU, low)):
        z_edges.append(plan(W.at[:, 0:D], ref.at[:, Y : Y + D], (0, -1, dz)))
        z_edges.append(plan(W.at[:, Y - D : Y], ref.at[:, YR - D : YR], (0, 1, dz)))
    for which in z_edges:
        start(which)
    start_near(y_faces[1])
    late_row = plan(V.at[:, 0:X, Y - M : Y - D], late, (0, 1, 0))
    start(late_row)
    if last_wave >= 2:
        announce(2)
    quarter = 0.5 * time_step
    zero8 = jnp.zeros((8, Z), jnp.float32)

    def split(f):
        return [f[8 * t : 8 * t + 8] for t in range(tiles)]

    def joined(ts):
        return jnp.concatenate(ts, axis=0)

    def up(f, by):
        return pltpu.roll(f, Z - by, 1)

    def down(f, by):
        return pltpu.roll(f, by, 1)

    def slide(f, by):
        return pltpu.roll(f, by % 8, 0)

    def rows_after(ts, last=0.0):
        r = [slide(t, -1) for t in ts] + [last]
        return [jnp.where(sub == 7, r[t + 1], r[t]) for t in range(len(ts))]

    def rows_before(ts, first=0.0):
        r = [first] + [slide(t, 1) for t in ts]
        return [jnp.where(sub == 0, r[t], r[t + 1]) for t in range(len(ts))]

    def inward(f):
        f = jnp.where(sub < M, slide(f, 1), slide(f, -1))
        return jnp.where((sub == 0) | (sub == 7), 0.0, f)

    def edge_of(seam, at):
        return pltpu.roll(seam, (Z - M) - 8 * at, 1)

    def seam_of(low_field, high_field):
        return jnp.where(low_lane, up(high_field, 1), down(low_field, 1))

    def planes_of(reach):
        own_planes = [(i, (i + 1) % XR, (i - 1) % XR, None) for i in range(X)]
        outer = []
        for j in range(reach):
            if one_sided:
                outer.append((
                    jnp.where(more, X + j, XR - 1 - j),
                    jnp.where(more, X + j + 1, (XR - j) % XR),
                    jnp.where(more, X + j - 1, XR - 2 - j),
                    None,
                ))
            else:
                for i in (X + j, -1 - j):
                    place = here[0] * X + i
                    xin = jnp.where((place >= 0) & (place < X * sizes[0]), 1.0, 0.0).astype(jnp.float32)
                    outer.append((i % XR, (i + 1) % XR, (i - 1) % XR, xin))
        return own_planes + outer

    def cut(value, xin):
        return value if xin is None else value * xin

    received(x_faces)
    for at, after, before, xin in planes_of(D):
        v = [split(V[c, at, 0:Y]) for c in range(comps)]
        va = [split(V[c, after, 0:Y]) for c in range(comps)]
        vb = [split(V[c, before, 0:Y]) for c in range(comps)]
        for c in range(comps):
            fy = [v[1][t] * v[c][t] for t in range(tiles)]
            ya, yb = rows_after(fy), rows_before(fy)
            YF[c, at] = jnp.where(sub == 7, slide(fy[0], -1), slide(fy[-1], 1))
            for t in range(tiles):
                fz = v[2][t] * v[c][t]
                total = va[0][t] * va[c][t] - vb[0][t] * vb[c][t]
                total = total + (ya[t] - yb[t])
                za = jnp.where(lane == Z - 1, 0.0, up(fz, 1))
                zb = jnp.where(lane == 0, 0.0, down(fz, 1))
                total = total + (za - zb)
                S0[c, at, 8 * t : 8 * t + 8] = cut(v[c][t] - quarter * total, xin)

    for wave in range(2, last_wave):
        heard(wave)
        announce(wave + 1)

    forwards = [
        plan(V.at[:, 0:M, Y:YR], V.at[:, X : X + M, Y:YR], (-1, 0, 0)),
        plan(V.at[:, X - M : X, Y:YR], V.at[:, X + M : XR, Y:YR], (1, 0, 0)),
    ]
    received(y_faces[0])
    start(forwards[1])
    start(forwards[0], jnp.logical_not(more))
    received(z_faces)

    masks = [mask_low[...], mask_high[...]]
    strip_v = [[], []]
    for t in range(tiles):
        at = slice(8 * t, 8 * t + 8)
        outer = (low[0, at], up(low[0, at], M), low[1, at])
        strip_v[0].append([jnp.where(low_lane, outer[c], PX[c, at]) for c in range(comps)])
        outer = (high[0, at], down(high[0, at], M), high[1, at])
        strip_v[1].append([jnp.where(low_lane, PX[c, at], outer[c]) for c in range(comps)])
    strips = [[[None] * comps for _ in range(4)] for _ in range(2)]
    for side in range(2):
        v = strip_v[side]
        inner = masks[side]
        for c in range(comps):
            fy = [v[t][1] * v[t][c] for t in range(tiles)]
            ya, yb = rows_after(fy), rows_before(fy)
            fields = [[], []]
            for t in range(tiles):
                fx, fz = v[t][0] * v[t][c], v[t][2] * v[t][c]
                total = up(fx, 8) - down(fx, 8)
                total = total + (ya[t] - yb[t])
                total = total + (up(fz, 1) - down(fz, 1))
                fields[0].append(fz)
                fields[1].append((v[t][c] - quarter * total) * inner)
            strips[side][0][c], strips[side][1][c] = fields
        for k in (2, 3):
            for c in range(comps):
                f = strips[side][k - 1][c]
                ya, yb = rows_after(f), rows_before(f)
                out = []
                for t in range(tiles):
                    total = (up(f[t], 8) + down(f[t], 8)) + (ya[t] + yb[t]) + (up(f[t], 1) + down(f[t], 1))
                    total = total * inner
                    out.append(total if k == 2 else total - 6.0 * strips[side][1][c][t])
                strips[side][k][c] = out

    def seams_of(k):
        return [[seam_of(strips[0][k][c][t], strips[1][k][c][t]) for t in range(tiles)] for c in range(comps)]

    flip = jnp.where(lane % 8 < M, quarter, -quarter)
    border = (lane == 0) | (lane == Z - 1)
    seam = [[s * flip for s in ts] for ts in seams_of(0)]
    for at, after, before, xin in planes_of(D):
        for c in range(comps):
            for t in range(tiles):
                edge = cut(edge_of(seam[c][t], at), xin)
                rows = slice(8 * t, 8 * t + 8)
                S0[c, at, rows] = S0[c, at, rows] - jnp.where(border, edge, 0.0)

    def around_tiles(ref, seam, c, at, after, before, first=0.0, last=0.0):
        f = split(ref[c, at])
        fa, fb = split(ref[c, after]), split(ref[c, before])
        ya, yb = rows_after(f, last), rows_before(f, first)
        out = []
        for t in range(tiles):
            edge = edge_of(seam[c][t], at)
            za = jnp.where(lane == Z - 1, edge, up(f[t], 1))
            zb = jnp.where(lane == 0, edge, down(f[t], 1))
            out.append((fa[t] + fb[t]) + (ya[t] + yb[t]) + (za + zb))
        return out

    seam = seams_of(1)
    for at, after, before, xin in planes_of(2):
        for c in range(comps):
            out = around_tiles(S0, seam, c, at, after, before)
            for t in range(tiles):
                S1[c, at, 8 * t : 8 * t + 8] = cut(out[t], xin)
    seam = seams_of(2)
    for at, after, before, xin in planes_of(1):
        for c in range(comps):
            out = around_tiles(S1, seam, c, at, after, before)
            for t in range(tiles):
                rows = slice(8 * t, 8 * t + 8)
                S2[c, at, rows] = cut(out[t], xin) - 6.0 * S0[c, at, rows]

    def from_tiles(first, last, by_first, by_last, at_first, at_last):
        return jnp.where(sub == at_last, slide(last, by_last), jnp.where(sub == at_first, slide(first, by_first), 0.0))

    def aligned(first, last):
        return jnp.where(sub < 3, slide(last, 3), jnp.where(sub > 4, slide(first, 5), 0.0))

    for at, after, before, xin in planes_of(2):
        for c in range(comps):
            P1[c, at] = cut(from_tiles(S0[c, at, 0:8], S0[c, at, Y - 8 : Y], 5, 3, 5, 2), xin)
    for at, after, before, xin in planes_of(1):
        for c in range(comps):
            P2[c, at] = cut(from_tiles(S1[c, at, 0:8], S1[c, at, Y - 8 : Y], 4, 4, 4, 3), xin)
    for i in range(X + 1):
        for c in range(comps):
            first, last = S2[c, i, 0:8], S2[c, i, Y - 8 : Y]
            A2[c, i] = aligned(first, last)
            if i < X:
                A0[c, i] = aligned(S0[c, i, 0:8], S0[c, i, Y - 8 : Y])
                A1[c, i] = aligned(S1[c, i, 0:8], S1[c, i, Y - 8 : Y])
                YA[c, i] = jnp.where((sub == 0) | (sub == 7), jnp.where(sub == 7, slide(first, 4), slide(last, 4)), 0.0)

    sums = [None] * (len(PAIRS) * comps)

    def add(c, full, kept):
        for k, (a, b) in enumerate(PAIRS):
            part = None
            for left, right in zip(kept[a], full[b]):
                part = left * right if part is None else part + left * right
            at = k * comps + c
            sums[at] = part if sums[at] is None else sums[at] + part

    crossing = (lane % 8 == M - 1) & (lane < 8 * X)
    last_tile = tiles - 1
    for i in range(X):
        for c in range(comps):
            full = [split(S[c, i]) for S in (S0, S1, S2)]
            f = full[2]
            fa = split(S2[c, i + 1])
            ya = rows_after(f)
            ya[last_tile] = jnp.where(sub < 4, ya[last_tile], 0.0)
            out = []
            for t in range(tiles):
                za = jnp.where(lane == Z - 1, 0.0, up(f[t], 1))
                out.append(fa[t] + ya[t] + za)
            kept = []
            for a in range(3):
                ts = list(full[a])
                ts[0] = jnp.where(sub >= 3, ts[0], 0.0)
                ts[last_tile] = jnp.where(sub < 5, ts[last_tile], 0.0)
                kept.append(ts)
            add(c, full + [out], kept)
            if i == 0:
                at = (len(PAIRS) - 1) * comps + c
                for t in range(tiles):
                    f = strips[1][3][c][t]
                    f = jnp.where(sub >= 3, f, 0.0) if t == 0 else f
                    f = jnp.where(sub < 5, f, 0.0) if t == last_tile else f
                    sums[at] = sums[at] + jnp.where(crossing, f * up(f, 1), 0.0)

    received(y_faces[1])
    start(forwards[0], more)
    received(forwards)
    received(z_edges)
    packed2 = []
    for c in range(comps):
        packed = zero8
        for x in range(XR):
            rolled = pltpu.roll(V[c, x, Y:YR], (8 * x + M) % Z, 1)
            packed = jnp.where(lane // 8 == x, rolled, packed)
        packed2.append(packed)

    ends = (sub == 0) | (sub == 7)
    signed = jnp.where(sub == 0, -quarter, quarter)

    def frame_of(center, corr):
        f = jnp.where(sub < M, slide(center, 1), slide(center, -1))
        return jnp.where(ends, corr, f)

    def frame_section(v2, end, c, fx_part, z_part, inner):
        fy2 = v2[1] * v2[c]
        ya = jnp.where(sub == 7, end, slide(fy2, -1))
        yb = jnp.where(sub == 0, end, slide(fy2, 1))
        value = (v2[c] - quarter * (fx_part + (ya - yb) + z_part)) * inner
        return frame_of(value, signed * fy2)

    at = slice(Y, YR)
    outer = (low[0, at], up(low[0, at], M), low[1, at])
    strip_v[0].append([jnp.where(low_lane, outer[c], packed2[c]) for c in range(comps)])
    outer = (high[0, at], down(high[0, at], M), high[1, at])
    strip_v[1].append([jnp.where(low_lane, packed2[c], outer[c]) for c in range(comps)])
    frames = [dict() for _ in range(2)]
    for side in range(2):
        v = strip_v[side]
        inner = masks[side] * frame_mask
        for c in range(comps):
            v2 = v[tiles]
            fx, fz = v2[0] * v2[c], v2[2] * v2[c]
            frames[side]["fz", c] = fz
            end = jnp.where(sub == 7, slide(v[0][1] * v[0][c], -1), slide(v[last_tile][1] * v[last_tile][c], 1))
            f0 = frame_section(v2, end, c, up(fx, 8) - down(fx, 8), up(fz, 1) - down(fz, 1), inner)
            f0 = jnp.where(ends, f0 * masks[side], f0)
            c0 = inward(f0)
            s = strips[side]
            f1 = (up(c0, 8) + down(c0, 8)) + (up(c0, 1) + down(c0, 1)) + f0 + inward(c0)
            f1 = (f1 + from_tiles(s[1][c][0], s[1][c][last_tile], 5, 3, 5, 2)) * inner
            c1 = inward(f1)
            f2 = (up(c1, 8) + down(c1, 8)) + (up(c1, 1) + down(c1, 1)) + f1 + inward(c1)
            f2 = (f2 + from_tiles(s[2][c][0], s[2][c][last_tile], 4, 4, 4, 3)) * inner - 6.0 * inward(c0)
            frames[side]["c0", c], frames[side]["c1", c], frames[side]["f2", c] = c0, c1, f2

    def frame_seam(name, c):
        return seam_of(frames[0][name, c], frames[1][name, c])

    seam = [frame_seam("fz", c) for c in range(comps)]
    for at, after, before, xin in planes_of(D):
        v2 = [V[c, at, Y:YR] for c in range(comps)]
        va = [V[c, after, Y:YR] for c in range(comps)]
        vb = [V[c, before, Y:YR] for c in range(comps)]
        for c in range(comps):
            fz = v2[2] * v2[c]
            edge = edge_of(seam[c], at)
            z_part = jnp.where(lane == Z - 1, edge, up(fz, 1)) - jnp.where(lane == 0, edge, down(fz, 1))
            f0 = frame_section(v2, YF[c, at], c, va[0] * va[c] - vb[0] * vb[c], z_part, frame_mask)
            f0 = cut(f0, xin)
            D0[c, at] = f0
            C0[c, at] = inward(f0)

    def around_frame(C, seam, c, at, after, before):
        f = C[c, at]
        edge = edge_of(seam[c], at)
        za = jnp.where(lane == Z - 1, edge, up(f, 1))
        zb = jnp.where(lane == 0, edge, down(f, 1))
        return (C[c, after] + C[c, before]) + (za + zb), inward(f)

    seam = [frame_seam("c0", c) for c in range(comps)]
    for at, after, before, xin in planes_of(2):
        for c in range(comps):
            f1, twice = around_frame(C0, seam, c, at, after, before)
            CC[c, at] = twice
            f1 = (cut(f1 + (twice + D0[c, at]), xin) + P1[c, at]) * frame_mask
            D1[c, at] = f1
            C1[c, at] = inward(f1)
    seam = [frame_seam("c1", c) for c in range(comps)]
    for at, after, before, xin in planes_of(1):
        for c in range(comps):
            f2, twice = around_frame(C1, seam, c, at, after, before)
            f2 = f2 + (twice + D1[c, at])
            D2[c, at] = (cut(f2, xin) + P2[c, at]) * frame_mask - 6.0 * CC[c, at]

    kept_rows = (sub < 3) | (sub > 4)

    for c in range(comps):
        f = frames[1]["f2", c] + aligned(strips[1][3][c][0], strips[1][3][c][last_tile])
        at = (len(PAIRS) - 1) * comps + c
        sums[at] = sums[at] + jnp.where(crossing & kept_rows, f * up(f, 1), 0.0)
    for i in range(X):
        for c in range(comps):
            full = [
                A0[c, i] + CC[c, i],
                A1[c, i] + C1[c, i],
                A2[c, i] + D2[c, i],
            ]
            f = full[2]
            fa = A2[c, i + 1] + D2[c, i + 1]
            ya = jnp.where(sub == 7, 0.0, slide(f, -1)) + YA[c, i]
            za = jnp.where(lane == Z - 1, 0.0, up(f, 1))
            full.append(fa + ya + za)
            kept = [[jnp.where(kept_rows, q, 0.0)] for q in full[:3]]
            add(c, [[q] for q in full], kept)

    line = jnp.zeros((8, Z), jnp.float32)
    several = [line] * 4
    for k, part in enumerate(sums):
        several[k % 4] = jnp.where(lane == k, jnp.sum(part, axis=1, keepdims=True), several[k % 4])
    line = (several[0] + several[1]) + (several[2] + several[3])
    line = jnp.sum(line, axis=0, keepdims=True)

    if last_wave >= 2:
        heard(last_wave)

    def residual_basis():
        received([late_row])

        def spread(ts, f):
            ts = list(ts)
            ts[0] = ts[0] + jnp.where(sub < 3, slide(f, 3), 0.0)
            ts[last_tile] = ts[last_tile] + jnp.where(sub > 4, slide(f, 5), 0.0)
            return ts

        seam = [[None] * tiles for _ in range(comps)]
        for c in range(comps):
            ends_of = [spread(strips[side][3][c], frames[side]["f2", c]) for side in range(2)]
            seam[c] = [seam_of(ends_of[0][t], ends_of[1][t]) for t in range(tiles)]
        for at, after, before, xin in planes_of(1):
            for c in range(comps):
                ts = spread(split(S2[c, at]), D2[c, at])
                for t in range(tiles):
                    S2[c, at, 8 * t : 8 * t + 8] = ts[t]
        for i, after, before, xin in planes_of(0):
            for c in range(comps):
                B0[c, i] = joined(spread(split(S0[c, i]), CC[c, i]))
                p1 = spread(split(S1[c, i]), C1[c, i])
                B1[c, i] = joined(p1)
                B2[c, i] = S2[c, i]
                beyond = slide(D2[c, i], 4)
                out = around_tiles(S2, seam, c, i, after, before, beyond, beyond)
                far = jnp.broadcast_to(quarter * (late[1, i] * late[c, i]), (8, Z))
                out[0] = out[0] + jnp.where(sub == 0, far, 0.0)
                B3[c, i] = joined([out[t] - 9.0 * p1[t] for t in range(tiles)])

    def added(terms):
        while len(terms) > 1:
            terms = [terms[k] + terms[k + 1] if k + 1 < len(terms) else terms[k] for k in range(0, len(terms), 2)]
        return terms[0]

    own_diff.wait()
    order = 0
    for group, landing in zip(groups, gathered):
        mine = slot_of(sizes, group)
        row[...] = line
        landing[mine] = line
        offsets = [o for o in peers if o in offsets_of(sizes, group)]
        for moved in offsets:
            pltpu.make_async_remote_copy(
                src_ref=row, dst_ref=landing.at[mine], send_sem=gs.at[order], recv_sem=gr.at[order],
                device_id=around(sizes, moved), device_id_type=MESH_IDS,
            ).start()
        if order == 0:
            residual_basis()
        many = landing.at[pl.ds(0, len(offsets))]
        pltpu.make_async_copy(many, many, gr.at[order]).wait()
        line = added([landing[k] for k in range(len(offsets) + 1)])
        pltpu.make_async_copy(many, many, gs.at[order]).wait()
        order += 1

    for c in range(comps):
        g = {}
        for k, (a, b) in enumerate(PAIRS):
            at = k * comps + c
            g[a, b] = g[b, a] = jnp.broadcast_to(line[:, at : at + 1], (1, Z))
        g[2, 3] = g[3, 2] = 2.0 * g[2, 3] - 9.0 * g[1, 2]
        g[0, 3] = g[1, 2] - 9.0 * g[0, 1]
        g[1, 3] = g[2, 2] + 6.0 * g[0, 2] - 9.0 * g[1, 1]
        coef = jnp.full((1, Z), diff_ref[c], jnp.float32)
        diagonal = 1.0 + 6.0 * coef

        def image_of(d):
            return [
                diagonal * d[0] - 6.0 * coef * d[1],
                diagonal * d[1] - coef * (d[0] + 9.0 * d[2]),
                diagonal * d[2] - coef * d[1],
                -coef * d[2],
            ]

        def form(a, b):
            terms = []
            for i, left in enumerate(a):
                inside = [right * g[i, j] for j, right in enumerate(b) if right is not zero]
                if left is not zero:
                    terms.append(left * added(inside))
            return added(terms)

        zero = jnp.zeros((1, Z), jnp.float32)
        res = [zero + 1.0, zero, zero, zero]
        direction = [zero + 1.0, zero, zero]
        found = [zero, zero, zero]
        norm = g[0, 0]
        inverse = 1.0 / norm
        for iteration in range(3):
            image = image_of(direction)
            if iteration == 0:
                image = [image[0], image[1], zero, zero]
            elif iteration == 1:
                image = [image[0], image[1], image[2], zero]
            step = norm / form(direction, image)
            found = [f if d is zero else f + step * d for f, d in zip(found, direction)]
            res = [r if m is zero else r - step * m for r, m in zip(res, image)]
            if iteration < 2:
                after = form(res[:3], res[:3])
                ratio = after * inverse
                inverse = 1.0 / after
                direction = [r if d is zero else r + ratio * d for r, d in zip(res, direction)]
                norm = after
        for k, value in enumerate(found + res):
            co_ref[8 * c + k : 8 * c + k + 1] = value

    for copy, moved in copies:
        pl.when(exists(moved))(copy.wait_send)


def combine(co_ref, B0, B1, B2, B3, x_hbm, r_hbm, x_ref, r_ref, sems):
    comps, X, Y, Z = B0.shape
    copies = []
    for c in range(comps):
        f = [jnp.broadcast_to(co_ref[8 * c + k : 8 * c + k + 1], (Y, Z)) for k in range(7)]
        for x in range(X):
            p = [B[c, x] for B in (B0, B1, B2, B3)]
            x_ref[c, x] = f[0] * p[0] + f[1] * p[1] + f[2] * p[2]
            r_ref[c, x] = f[3] * p[0] + f[4] * p[1] + f[5] * p[2] + f[6] * p[3]
        for k, (src, dst) in enumerate(((x_ref, x_hbm), (r_ref, r_hbm))):
            copy = pltpu.make_async_copy(src.at[c], dst.at[c], sems.at[k, c])
            copy.start()
            copies.append(copy)
    for copy in copies:
        copy.wait()


def solution(mesh):
    sizes = tuple(mesh.shape[a] for a in AXES)
    groups = groups_of(sizes)

    def body(velocity, diffusion):
        comps, X, Y, Z = velocity.shape
        XR, YR = X + 2 * MARGIN, Y + 2 * MARGIN
        assert X == 2 * MARGIN and XR * 8 == Z and MARGIN * 2 == 8
        f32 = jnp.float32
        whole = pltpu.VMEM((comps, XR, YR, Z), f32)
        packed = pltpu.VMEM((comps + 2, Y, Z), f32)
        inner = pltpu.VMEM((comps, XR, Y, Z), f32)
        frame = pltpu.VMEM((comps, XR, 8, Z), f32)
        strip = pltpu.VMEM((comps, YR, Z), f32)
        counts = [len(offsets_of(sizes, group)) + 1 for group in groups]
        out = pltpu.VMEM(velocity.shape, f32)
        vmem = pl.BlockSpec(memory_space=pltpu.VMEM)
        hbm = pl.BlockSpec(memory_space=pltpu.HBM)
        basis = pl.pallas_call(
            functools.partial(kernel, sizes),
            out_shape=(out, out, out, out, pltpu.VMEM((8 * comps, Z), f32)),
            in_specs=[hbm] * 2,
            out_specs=(vmem,) * 5,
            scratch_shapes=[
                pltpu.SMEM((comps,), f32),
                whole, inner, inner, inner,
                *[frame] * 13,
                pltpu.VMEM((comps, X, 1, Z), f32),
                packed, packed, packed, packed, strip,
                pltpu.VMEM((2, Y, Z), f32), pltpu.VMEM((2, Y, Z), f32),
                pltpu.VMEM((2, YR, Z), f32), pltpu.VMEM((2, YR, Z), f32),
                pltpu.VMEM((8, Z), f32),
                pltpu.VMEM((8, Z), f32),
                pltpu.VMEM((1, Z), f32),
                *[pltpu.VMEM((count, 1, Z), f32) for count in counts],
                pltpu.SemaphoreType.DMA((17,)),
                pltpu.SemaphoreType.DMA((17,)),
                pltpu.SemaphoreType.DMA((len(groups),)),
                pltpu.SemaphoreType.DMA((len(groups),)),
                pltpu.SemaphoreType.DMA((2,)),
                pltpu.SemaphoreType.REGULAR((sizes[2] + 1, 2)),
            ],
            compiler_params=pltpu.CompilerParams(collective_id=0, has_side_effects=True, vmem_limit_bytes=GRANT),
        )(diffusion, velocity)
        shape = jax.ShapeDtypeStruct(velocity.shape, f32)
        return pl.pallas_call(
            combine,
            out_shape=(shape, shape),
            in_specs=[vmem] * 5,
            out_specs=(hbm, hbm),
            scratch_shapes=[
                pltpu.VMEM(velocity.shape, f32),
                pltpu.VMEM(velocity.shape, f32),
                pltpu.SemaphoreType.DMA((2, comps)),
            ],
            compiler_params=pltpu.CompilerParams(vmem_limit_bytes=SMALL),
        )(basis[4], *basis[:4])

    return jax.shard_map(
        body,
        mesh=mesh,
        in_specs=(P(None, "gx", "gy", "gz"), P()),
        out_specs=(P(None, "gx", "gy", "gz"), P(None, "gx", "gy", "gz")),
        check_vma=False,
    )
```
